8 devices in a mesh: dp: 2 (over z, y), tp: 4 (over x, core).
Axes of the slice: x: 2, y: 2, z: 1, core: 2. Of those that a mesh axis runs over, the one named last changes fastest.
Arguments:
- hidden: bfloat16 [2, 256, 5120], P('dp', 'tp'), parts along dimension 0
- attn_gain: float32 [5120], replicated
- attn_bias: float32 [5120], replicated
- mlp_gain: float32 [5120], replicated
- mlp_bias: float32 [5120], replicated
- w_qkv: bfloat16 [5120, 40, 384], P(None, 'tp')
- w_out: bfloat16 [5120, 5120], P('tp')
- w_up: bfloat16 [5120, 20480], P(None, 'tp')
- w_down: bfloat16 [20480, 5120], P('tp')
- positions: int32 [256], replicated
Outputs:
- output: bfloat16 [2, 256, 5120], P('dp', 'tp'), parts along dimension 0
There are 2 independent parts. The reference program is written for one: setup_inputs(seed, part) draws one part's arguments, and reference() takes and returns one part's arrays. A program takes and returns all parts, laid end to end along the dimension named above; an argument that names none is the same for every part.
All inputs are finite; a program needn't handle non-finite values.
Results may differ from the reference program's by a relative error of at most 0.00364416.
Values are sent between devices in bfloat16 or wider.
A program may use at most 1 GiB of HBM per device.

```python
import jax
import jax.numpy as jnp
from jax import lax

D = 5120
HEADS = 40
KV_HEADS = 40
HEAD = 128
FF = 20480
BATCH = 1
SEQ_LEN = 256
QUERY_BLOCK = 64
HALF_HEAD = 64

GROUP_SIZE = HEADS // KV_HEADS
QKV_COLS = (GROUP_SIZE + 2) * HEAD


def setup_inputs(seed: int = 0, part: int = 0) -> dict:
    root_key = jax.random.key(seed)
    sub_keys = jax.random.split(root_key, 10)
    part_key = jax.random.fold_in(sub_keys[0], part)
    hidden = jax.random.normal(part_key, (BATCH, SEQ_LEN, D), jnp.float32).astype(jnp.bfloat16)
    attn_gain = 1.0 + 0.4 * jax.random.normal(sub_keys[1], (D,), jnp.float32)
    attn_bias = 0.4 * jax.random.normal(sub_keys[2], (D,), jnp.float32)
    mlp_gain = 1.0 + 0.4 * jax.random.normal(sub_keys[3], (D,), jnp.float32)
    mlp_bias = 0.4 * jax.random.normal(sub_keys[4], (D,), jnp.float32)
    w_qkv = (1.2 * D ** -0.5 * jax.random.normal(sub_keys[5], (D, KV_HEADS, QKV_COLS), jnp.float32)).astype(jnp.bfloat16)
    w_out = (2.0 * (HEADS * HEAD) ** -0.5 * jax.random.normal(sub_keys[6], (HEADS * HEAD, D), jnp.float32)).astype(jnp.bfloat16)
    w_up = (D ** -0.5 * jax.random.normal(sub_keys[7], (D, FF), jnp.float32)).astype(jnp.bfloat16)
    w_down = (FF ** -0.5 * jax.random.normal(sub_keys[8], (FF, D), jnp.float32)).astype(jnp.bfloat16)
    pos_gaps = jax.random.randint(sub_keys[9], (SEQ_LEN,), 1, 4, jnp.int32)
    positions = (jnp.cumsum(pos_gaps) - pos_gaps[0]).astype(jnp.int32)
    return {'hidden': hidden, 'attn_gain': attn_gain, 'attn_bias': attn_bias, 'mlp_gain': mlp_gain, 'mlp_bias': mlp_bias, 'w_qkv': w_qkv, 'w_out': w_out, 'w_up': w_up, 'w_down': w_down, 'positions': positions}


def layer_norm(tok_rows, norm_gain, norm_bias):
    rows32 = tok_rows.astype(jnp.float32)
    row_mean = jnp.mean(rows32, axis=-1, keepdims=True)
    centered = rows32 - row_mean
    row_var = jnp.mean(centered * centered, axis=-1, keepdims=True)
    return (centered * lax.rsqrt(row_var + 1e-5) * norm_gain + norm_bias).astype(jnp.bfloat16)


def apply_rotary(head_vals, cos_tab, sin_tab):
    vals32 = head_vals.astype(jnp.float32)
    rotated = jnp.concatenate([-vals32[..., HALF_HEAD:], vals32[..., :HALF_HEAD]], axis=-1)
    return (vals32 * cos_tab + rotated * sin_tab).astype(jnp.bfloat16)


def attend_sequence(query_rot, key_rot, value_seq):
    key32 = key_rot.astype(jnp.float32)
    value32 = value_seq.astype(jnp.float32)
    key_idx = jnp.arange(SEQ_LEN)

    def one_block(block_idx):
        row_start = block_idx * QUERY_BLOCK
        query_blk = lax.dynamic_slice_in_dim(query_rot, row_start, QUERY_BLOCK, axis=0).astype(jnp.float32)
        scores = jnp.einsum('qkgh,skh->kgqs', query_blk, key32) * HEAD ** -0.5
        query_idx = row_start + jnp.arange(QUERY_BLOCK)
        allowed = key_idx[None, :] <= query_idx[:, None]
        scores = jnp.where(allowed, scores, -1e30)
        exp_scores = jnp.exp(scores - jnp.max(scores, axis=-1, keepdims=True))
        attn_probs = (exp_scores / jnp.sum(exp_scores, axis=-1, keepdims=True)).astype(jnp.bfloat16)
        context = jnp.einsum('kgqs,skh->qkgh', attn_probs.astype(jnp.float32), value32)
        return context.astype(jnp.bfloat16)

    ctx_blocks = lax.map(one_block, jnp.arange(SEQ_LEN // QUERY_BLOCK))
    return ctx_blocks.reshape(SEQ_LEN, HEADS * HEAD)


def reference(hidden, attn_gain, attn_bias, mlp_gain, mlp_bias, w_qkv, w_out, w_up, w_down, positions):
    inv_freq = 10000.0 ** (-2.0 * jnp.arange(HALF_HEAD, dtype=jnp.float32) / HEAD)
    angles = positions.astype(jnp.float32)[:, None] * inv_freq[None, :]
    angles = jnp.concatenate([angles, angles], axis=-1)
    cos_tab = jnp.cos(angles)
    sin_tab = jnp.sin(angles)
    w_qkv_flat = w_qkv.reshape(D, KV_HEADS * QKV_COLS)

    def one_sequence(seq_rows):
        normed_attn = layer_norm(seq_rows, attn_gain, attn_bias)
        normed_mlp = layer_norm(seq_rows, mlp_gain, mlp_bias)
        qkv_rows = jnp.dot(normed_attn, w_qkv_flat, preferred_element_type=jnp.float32).astype(jnp.bfloat16)
        qkv_rows = qkv_rows.reshape(SEQ_LEN, KV_HEADS, GROUP_SIZE + 2, HEAD)
        query_rot = apply_rotary(qkv_rows[:, :, :GROUP_SIZE, :], cos_tab[:, None, None, :], sin_tab[:, None, None, :])
        key_rot = apply_rotary(qkv_rows[:, :, GROUP_SIZE, :], cos_tab[:, None, :], sin_tab[:, None, :])
        value_seq = qkv_rows[:, :, GROUP_SIZE + 1, :]
        context = attend_sequence(query_rot, key_rot, value_seq)
        attn_part = jnp.dot(context, w_out, preferred_element_type=jnp.float32)
        up_pre = jnp.dot(normed_mlp, w_up, preferred_element_type=jnp.float32)
        up_act = jax.nn.gelu(up_pre, approximate=False).astype(jnp.bfloat16)
        mlp_part = jnp.dot(up_act, w_down, preferred_element_type=jnp.float32)
        return (seq_rows.astype(jnp.float32) + attn_part + mlp_part).astype(jnp.bfloat16)

    return lax.map(one_sequence, hidden)
```

```python
import jax
import jax.numpy as jnp
from jax import lax
from jax.experimental import pallas as pl
from jax.experimental.pallas import tpu as pltpu
from jax.sharding import PartitionSpec as P

MESH = pl.DeviceIdType.MESH
F32 = jnp.float32
BF16 = jnp.bfloat16

D = 5120
T = 256
TB = 64
HD = 128
G = 10
FF = 5120
NB = 512
CTX = G * HD
RING = 6
WORING = 3
N_UP = FF // NB
N_V = 3
N_QK = G // 2
N_DN = D // NB
V0 = N_UP
QK0 = V0 + N_V
DN0 = QK0 + N_QK
N_ITEMS = DN0 + N_DN
NPIECE = 4
PROWS = TB // NPIECE


def body(x_hbm, ga_hbm, ba_hbm, gm_hbm, bm_hbm, wqkv_hbm, wo_hbm, wup_hbm, wdn_hbm, pos_hbm,
         out_hbm,
         xall, a_all, m_all, act, ctx, v_all, acc, cos_t, sin_t, norms, pos_v,
         ring, woring, part, ra, sb, rb, outv,
         ring_sem, wo_sem, misc_sem, x_send, x_recv, c_send, c_recv, f_send, f_recv,
         a_send, a_recv, b_send, b_recv, out_sem):
    t = lax.axis_index("tp")
    partner = t + 1 - 2 * lax.rem(t, 2)
    cross = lax.rem(t + 2, 4)
    diag = lax.rem(partner + 2, 4)

    def local(src, dst, sem):
        return pltpu.make_async_copy(src, dst, sem)

    def remote(src, dst, ssem, rsem, dev):
        return pltpu.make_async_remote_copy(src_ref=src, dst_ref=dst, send_sem=ssem, recv_sem=rsem,
                                            device_id={"tp": dev}, device_id_type=MESH)

    def cols(i, n=NB):
        return pl.ds(pl.multiple_of(i * n, n), n)

    def issue_up(g):
        s = lax.rem(g, RING)
        local(wup_hbm.at[:, cols(g)], ring.at[s], ring_sem.at[s]).start()

    def issue_v(j, s):
        for h in range(4 if j < 2 else 2):
            local(wqkv_hbm.at[4 * j + h, :, pl.ds(2 * HD, HD)], ring.at[s, :, pl.ds(h * HD, HD)], ring_sem.at[s]).start()

    def issue_qk(g):
        s = lax.rem(g, RING)
        j = g - QK0
        for h in range(2):
            local(wqkv_hbm.at[2 * j + h, :, pl.ds(0, 2 * HD)], ring.at[s, :, pl.ds(h * 2 * HD, 2 * HD)], ring_sem.at[s]).start()

    def issue_dn(g):
        s = lax.rem(g, RING)
        j = g - DN0
        local(wdn_hbm.at[:, cols(j)], ring.at[s], ring_sem.at[s]).start()

    def issue_wo(j):
        w = lax.rem(j, WORING)
        local(wo_hbm.at[:, cols(j)], woring.at[w], wo_sem.at[w]).start()

    def issue(g):
        @pl.when(g < V0)
        def _():
            issue_up(g)
        for j in range(N_V):
            @pl.when(g == V0 + j)
            def _(j=j):
                issue_v(j, (V0 + j) % RING)

        @pl.when(jnp.logical_and(g >= QK0, g < DN0))
        def _():
            issue_qk(g)

        @pl.when(jnp.logical_and(g >= DN0, g < N_ITEMS))
        def _():
            issue_dn(g)

    def wait_ring(g):
        s = lax.rem(g, RING)
        local(wup_hbm.at[:, pl.ds(0, NB)], ring.at[s], ring_sem.at[s]).wait()
        return s

    xc = local(x_hbm, xall.at[t], misc_sem.at[0])
    xc.start()
    small = [local(h, norms.at[pl.ds(i, 1), :], misc_sem.at[1 + i]) for i, h in enumerate((ga_hbm, ba_hbm, gm_hbm, bm_hbm))]
    small.append(local(pos_hbm, pos_v, misc_sem.at[5]))
    for c in small:
        c.start()
    barrier = pltpu.get_barrier_semaphore()
    for dev in (partner, cross):
        pl.semaphore_signal(barrier, inc=1, device_id={"tp": dev}, device_id_type=MESH)
    for g in range(RING):
        issue_up(g)
    pl.semaphore_wait(barrier, 2)
    xc.wait()

    def piece(i):
        return pl.ds(i * PROWS, PROWS)

    to_cross = [remote(xall.at[t, piece(i)], xall.at[t, piece(i)], c_send.at[i], c_recv.at[i], cross) for i in range(NPIECE)]
    for c in to_cross:
        c.start()
    to_partner = remote(xall.at[t], xall.at[t], x_send.at[0], x_recv.at[0], partner)
    to_partner.start()
    from_cross = [remote(xall.at[cross, piece(i)], xall.at[cross, piece(i)], c_send.at[i], c_recv.at[i], cross) for i in range(NPIECE)]
    from_partner = remote(xall.at[partner], xall.at[partner], x_send.at[0], x_recv.at[0], partner)
    forward = [remote(xall.at[cross, piece(i)], xall.at[cross, piece(i)], f_send.at[i], f_recv.at[i], partner) for i in range(NPIECE)]
    from_fwd = [remote(xall.at[diag, piece(i)], xall.at[diag, piece(i)], f_send.at[i], f_recv.at[i], partner) for i in range(NPIECE)]

    for c in small:
        c.wait()

    lane = lax.broadcasted_iota(jnp.int32, (HD, T), 0)
    half = jnp.where(lane < HD // 2, lane, lane - HD // 2).astype(F32)
    inv_freq = jnp.exp(half * (-2.0 / HD) * 9.210340371976184)
    ang = pos_v[...].astype(F32) * inv_freq
    cos_t[...] = jnp.cos(ang).T
    sin_t[...] = jnp.where(lane < HD // 2, -jnp.sin(ang), jnp.sin(ang)).T
    acc[...] = jnp.zeros_like(acc)

    LR = 16

    def norm_rows(blk, row0):
        xr = xall[blk, pl.ds(row0, LR), :].astype(F32)
        mean = jnp.mean(xr, axis=-1, keepdims=True)
        cen = xr - mean
        var = jnp.mean(cen * cen, axis=-1, keepdims=True)
        z = cen * lax.rsqrt(var + 1e-5)
        dst = pl.ds(pl.multiple_of(blk * TB + row0, LR), LR)
        a_all[dst, :] = (z * norms[0:1, :] + norms[1:2, :]).astype(BF16)
        m_all[dst, :] = (z * norms[2:3, :] + norms[3:4, :]).astype(BF16)

    def norm_block(blk, start, n):
        def step(i, carry):
            norm_rows(blk, pl.multiple_of(start + i * LR, LR))
            return carry
        lax.fori_loop(0, n // LR, step, 0)

    norm_block(t, 0, TB)
    from_partner.wait_recv()
    norm_block(partner, 0, TB)
    for i in range(NPIECE):
        from_cross[i].wait_recv()
        forward[i].start()
        norm_block(cross, i * PROWS, PROWS)
        if i:
            from_fwd[i - 1].wait_recv()
            norm_block(diag, (i - 1) * PROWS, PROWS)
    from_fwd[NPIECE - 1].wait_recv()
    norm_block(diag, (NPIECE - 1) * PROWS, PROWS)

    def gelu_store(j):
        u = acc[...]
        act[:, cols(j)] = (0.5 * u * (1.0 + lax.erf(u * 0.7071067811865476))).astype(BF16)

    def up_step(g, carry):
        s = wait_ring(g)

        @pl.when(g >= 1)
        def _():
            issue(g + RING - 1)
        gelu_store(jnp.maximum(g - 1, 0))
        acc[...] = jnp.dot(m_all[...], ring[s], preferred_element_type=F32)
        return carry

    lax.fori_loop(0, N_UP, up_step, 0)

    for j in range(N_V):
        g = V0 + j
        s = g % RING
        n = NB if j < 2 else NB // 2
        local(wup_hbm.at[:, pl.ds(0, n)], ring.at[s, :, pl.ds(0, n)], ring_sem.at[s]).wait()
        issue(jnp.int32(g + RING - 1))
        if j == 0:
            gelu_store(N_UP - 1)
        v_all[:, pl.ds(j * NB, n)] = jnp.dot(a_all[...], ring[s, :, pl.ds(0, n)], preferred_element_type=F32).astype(BF16)

    def attend(j):
        def rot(u):
            u = u.astype(BF16).astype(F32)
            return (u * cos_t[...] + pltpu.roll(u, HD // 2, 1) * sin_t[...]).astype(BF16)

        mask = lax.broadcasted_iota(jnp.int32, (T, T), 1) <= lax.broadcasted_iota(jnp.int32, (T, T), 0)
        for h in range(2):
            q = rot(acc[:, pl.ds(2 * h * HD, HD)])
            k = rot(acc[:, pl.ds((2 * h + 1) * HD, HD)])
            hcol = pl.ds(pl.multiple_of((2 * j + h) * HD, HD), HD)
            v = v_all[:, hcol]
            sc = lax.dot_general(q, k, (((1,), (1,)), ((), ())), preferred_element_type=F32) * (HD ** -0.5)
            sc = jnp.where(mask, sc, -1e30)
            e = jnp.exp(sc - jnp.max(sc, axis=-1, keepdims=True))
            p = (e * (1.0 / jnp.sum(e, axis=-1, keepdims=True))).astype(BF16)
            ctx[:, hcol] = jnp.dot(p, v, preferred_element_type=F32).astype(BF16)

    acc[...] = jnp.zeros_like(acc)
    for j in range(WORING - 1):
        issue_wo(j)

    def qk_step(g, carry):
        s = wait_ring(g)
        issue(g + RING - 1)
        attend(jnp.maximum(g - QK0 - 1, 0))
        acc[...] = jnp.dot(a_all[...], ring[s], preferred_element_type=F32)
        return carry

    lax.fori_loop(QK0, DN0, qk_step, 0)
    attend(N_QK - 1)

    def rows(blk):
        return pl.ds(pl.multiple_of(blk * TB, TB), TB)

    def a_copy(j, i):
        blk = partner if i == 0 else diag
        return remote(part.at[j, rows(blk)], ra.at[j, i], a_send.at[j, i], a_recv.at[j, i], partner)

    def b_copy(j):
        return remote(sb.at[j], rb.at[j], b_send.at[j], b_recv.at[j], cross)

    def do_a(j):
        for i in range(2):
            a_copy(j, i).start()

    def do_b(j):
        for i in range(2):
            a_copy(j, i).wait_recv()
        sb[j] = (part[j, rows(cross), :] + ra[j, 1]).astype(BF16)
        b_copy(j).start()

    def out_copy(j):
        return local(outv.at[:, cols(j)], out_hbm.at[:, cols(j)], out_sem.at[j])

    def do_c(j):
        b_copy(j).wait_recv()
        tot = (part[j, rows(t), :] + ra[j, 0]) + rb[j].astype(F32)
        outv[:, cols(j)] = (xall[t, :, cols(j)].astype(F32) + tot).astype(BF16)
        out_copy(j).start()

    def dn_step(j, carry):
        g = j + DN0
        s = wait_ring(g)
        w = lax.rem(j, WORING)
        local(wo_hbm.at[:, pl.ds(0, NB)], woring.at[w], wo_sem.at[w]).wait()

        @pl.when(j >= 1)
        def _():
            do_a(j - 1)

        @pl.when(j + DN0 + RING - 1 < N_ITEMS)
        def _():
            issue(g + RING - 1)

        @pl.when(j + WORING - 1 < N_DN)
        def _():
            issue_wo(j + WORING - 1)

        @pl.when(j >= 2)
        def _():
            do_b(j - 2)

        @pl.when(j >= 4)
        def _():
            do_c(j - 4)
        part[j] = jnp.dot(act[...], ring[s], preferred_element_type=F32) + jnp.dot(ctx[...], woring[w], preferred_element_type=F32)
        return carry

    lax.fori_loop(0, N_DN, dn_step, 0)
    do_a(N_DN - 1)
    do_b(N_DN - 2)
    do_c(N_DN - 4)
    do_b(N_DN - 1)
    for j in range(N_DN - 3, N_DN):
        do_c(j)

    for c in to_cross + [to_partner] + forward:
        c.wait_send()

    def drain(j, carry):
        for i in range(2):
            a_copy(j, i).wait_send()
        b_copy(j).wait_send()
        out_copy(j).wait()
        return carry

    lax.fori_loop(0, N_DN, drain, 0)


def solution(mesh):
    def local_layer(hidden_blk, attn_gain, attn_bias, mlp_gain, mlp_bias, w_qkv, w_out, w_up, w_down, positions):
        args = (hidden_blk.reshape(TB, D), attn_gain.reshape(1, D), attn_bias.reshape(1, D), mlp_gain.reshape(1, D),
                mlp_bias.reshape(1, D), jnp.transpose(w_qkv, (1, 0, 2)), w_out, w_up, w_down, positions.reshape(1, T))
        dma = pltpu.SemaphoreType.DMA
        out = pl.pallas_call(
            body,
            out_shape=jax.ShapeDtypeStruct((TB, D), BF16),
            in_specs=[pl.BlockSpec(memory_space=pl.ANY)] * 10,
            out_specs=pl.BlockSpec(memory_space=pl.ANY),
            scratch_shapes=[
                pltpu.VMEM((4, TB, D), BF16),
                pltpu.VMEM((T, D), BF16),
                pltpu.VMEM((T, D), BF16),
                pltpu.VMEM((T, FF), BF16),
                pltpu.VMEM((T, CTX), BF16),
                pltpu.VMEM((T, CTX), BF16),
                pltpu.VMEM((T, NB), F32),
                pltpu.VMEM((T, HD), F32),
                pltpu.VMEM((T, HD), F32),
                pltpu.VMEM((4, D), F32),
                pltpu.VMEM((1, T), jnp.int32),
                pltpu.VMEM((RING, D, NB), BF16),
                pltpu.VMEM((WORING, CTX, NB), BF16),
                pltpu.VMEM((N_DN, T, NB), F32),
                pltpu.VMEM((N_DN, 2, TB, NB), F32),
                pltpu.VMEM((N_DN, TB, NB), BF16),
                pltpu.VMEM((N_DN, TB, NB), BF16),
                pltpu.VMEM((TB, D), BF16),
                dma((RING,)), dma((WORING,)), dma((6,)), dma((1,)), dma((1,)), dma((NPIECE,)), dma((NPIECE,)),
                dma((NPIECE,)), dma((NPIECE,)), dma((N_DN, 2)), dma((N_DN, 2)), dma((N_DN,)), dma((N_DN,)), dma((N_DN,)),
            ],
            compiler_params=pltpu.CompilerParams(collective_id=0, has_side_effects=True, vmem_limit_bytes=67043328),
            cost_estimate=pl.CostEstimate(flops=40_300_000_000, bytes_accessed=158_000_000, transcendentals=2_000_000),
            name="layer",
        )(*args)
        return out.reshape(1, TB, D)

    return jax.shard_map(local_layer, mesh=mesh,
                         in_specs=(P('dp', 'tp', None), P(), P(), P(), P(), P(None, 'tp', None), P('tp', None), P(None, 'tp'), P('tp', None), P()),
                         out_specs=P('dp', 'tp', None), check_vma=False)
```

```python
import jax
import jax.numpy as jnp
from jax import lax
from jax.experimental import pallas as pl
from jax.experimental.pallas import tpu as pltpu
from jax.sharding import PartitionSpec as P

MESH = pl.DeviceIdType.MESH
F32 = jnp.float32
BF16 = jnp.bfloat16

D = 5120
T = 256
TB = 64
HD = 128
G = 10
FF = 5120
NB = 512
CTX = G * HD
RING = 9
WORING = 2
N_QKV = 8
N_UP = FF // NB
N_DN = D // NB
UP0 = N_QKV
DN0 = UP0 + N_UP
N_ITEMS = DN0 + N_DN
NPIECE = 4
PROWS = TB // NPIECE
HALF = 2 * TB
RA = 4
KC = 2560


def body(x_hbm, ga_hbm, ba_hbm, gm_hbm, bm_hbm, wqkv_hbm, wo_hbm, wup_hbm, wdn_hbm, pos_hbm,
         out_hbm,
         x_own, abuf, ctx, acc, norms, pos_v,
         ring, woring, ra, sb, rb, out_v,
         ring_sem, wo_sem, misc_sem, x_send, x_recv, c_send, c_recv, f_send, f_recv,
         a_send, a_recv, b_send, b_recv, out_sem):
    t = lax.axis_index("tp")
    partner = t + 1 - 2 * lax.rem(t, 2)
    cross = lax.rem(t + 2, 4)
    diag = lax.rem(partner + 2, 4)
    near0 = pl.multiple_of((t // 2) * HALF, HALF)
    far0 = pl.multiple_of((1 - t // 2) * HALF, HALF)

    def local(src, dst, sem):
        return pltpu.make_async_copy(src, dst, sem)

    def remote(src, dst, ssem, rsem, dev):
        return pltpu.make_async_remote_copy(src_ref=src, dst_ref=dst, send_sem=ssem, recv_sem=rsem,
                                            device_id={"tp": dev}, device_id_type=MESH)

    def rows(blk, start=0, n=TB):
        return pl.ds(pl.multiple_of(blk * TB + start, 16), n)

    def cols(i, n=NB):
        return pl.ds(pl.multiple_of(i * n, n), n)

    def issue_qkv(p):
        if p in (0, 1, 7):
            j = {0: 0, 1: 1, 7: 2}[p]
            for h in range(4 if j < 2 else 2):
                local(wqkv_hbm.at[4 * j + h, :, pl.ds(2 * HD, HD)], ring.at[p, :, pl.ds(h * HD, HD)], ring_sem.at[p]).start()
        else:
            for h in range(2):
                local(wqkv_hbm.at[2 * (p - 2) + h, :, pl.ds(0, 2 * HD)], ring.at[p, :, pl.ds(h * 2 * HD, 2 * HD)], ring_sem.at[p]).start()

    def issue(g):
        s = lax.rem(g, RING)

        @pl.when(g < DN0)
        def _():
            local(wup_hbm.at[:, cols(g - UP0)], ring.at[s], ring_sem.at[s]).start()

        @pl.when(jnp.logical_and(g >= DN0, g < N_ITEMS))
        def _():
            local(wdn_hbm.at[:, cols(g - DN0)], ring.at[s], ring_sem.at[s]).start()

    def issue_wo(j):
        w = lax.rem(j, WORING)
        local(wo_hbm.at[:, cols(j)], woring.at[w], wo_sem.at[w]).start()

    def wait_ring(g, n=NB):
        s = lax.rem(g, RING)
        local(wup_hbm.at[:, pl.ds(0, n)], ring.at[s, :, pl.ds(0, n)], ring_sem.at[s]).wait()
        return s

    xc = local(x_hbm, x_own, misc_sem.at[0])
    xc.start()
    small = [local(h, norms.at[pl.ds(i, 1), :], misc_sem.at[1 + i]) for i, h in enumerate((ga_hbm, ba_hbm, gm_hbm, bm_hbm))]
    small.append(local(pos_hbm, pos_v, misc_sem.at[5]))
    for c in small:
        c.start()
    barrier = pltpu.get_barrier_semaphore()
    for dev in (partner, cross):
        pl.semaphore_signal(barrier, inc=1, device_id={"tp": dev}, device_id_type=MESH)
    for p in range(N_QKV):
        issue_qkv(p)
    issue(jnp.int32(UP0))
    xc.wait()
    pl.semaphore_wait(barrier, 2)

    to_cross = [remote(x_own.at[pl.ds(i * PROWS, PROWS)], abuf.at[rows(t, i * PROWS, PROWS)], c_send.at[i], c_recv.at[i], cross) for i in range(NPIECE)]
    for c in to_cross:
        c.start()
    to_partner = remote(x_own, abuf.at[rows(t)], x_send.at[0], x_recv.at[0], partner)
    to_partner.start()

    def cross_rows(i):
        return abuf.at[rows(cross, i * PROWS, PROWS)]

    def diag_rows(i):
        return abuf.at[rows(diag, i * PROWS, PROWS)]

    from_cross = [remote(cross_rows(i), cross_rows(i), c_send.at[i], c_recv.at[i], cross) for i in range(NPIECE)]
    from_partner = remote(abuf.at[rows(partner)], abuf.at[rows(partner)], x_send.at[0], x_recv.at[0], partner)
    forward = [remote(cross_rows(i), cross_rows(i), f_send.at[i], f_recv.at[i], partner) for i in range(NPIECE)]
    from_fwd = [remote(diag_rows(i), diag_rows(i), f_send.at[i], f_recv.at[i], partner) for i in range(NPIECE)]

    def gelu_store(j):
        u = acc[...]
        abuf[:, cols(j)] = (0.5 * u * (1.0 + lax.erf(u * 0.7071067811865476))).astype(BF16)

    def front(m_all, qkv, cos_t, sin_t):
        LR = 16

        def norm_rows(src, r_src, r_dst):
            xr = src[r_src, :].astype(F32)
            mean = jnp.mean(xr, axis=-1, keepdims=True)
            cen = xr - mean
            var = jnp.mean(cen * cen, axis=-1, keepdims=True)
            z = cen * lax.rsqrt(var + 1e-5)
            abuf[r_dst, :] = (z * norms[0:1, :] + norms[1:2, :]).astype(BF16)
            m_all[r_dst, :] = (z * norms[2:3, :] + norms[3:4, :]).astype(BF16)

        for c in small:
            c.wait()

        def own_step(i, carry):
            norm_rows(x_own, pl.ds(pl.multiple_of(i * LR, LR), LR), rows(t, i * LR, LR))
            return carry

        lax.fori_loop(0, TB // LR, own_step, 0)
        from_partner.wait_recv()

        def blk_step(i, carry):
            r = rows(partner, i * LR, LR)
            norm_rows(abuf, r, r)
            return carry

        lax.fori_loop(0, TB // LR, blk_step, 0)

        def norm_piece(blk, i):
            r = rows(blk, i * PROWS, PROWS)
            norm_rows(abuf, r, r)

        def qkv_half(p, r0):
            r = pl.ds(r0, HALF)
            qkv[p, r, :] = jnp.dot(abuf[r, :], ring[p], preferred_element_type=F32).astype(BF16)

        def qkv_last(r0):
            r = pl.ds(r0, HALF)
            p = N_QKV - 1
            n = NB // 2
            qkv[p, r, pl.ds(0, n)] = jnp.dot(abuf[r, :], ring[p, :, pl.ds(0, n)], preferred_element_type=F32).astype(BF16)

        def near_step(p, carry):
            wait_ring(p)

            @pl.when(p == 3)
            def _():
                from_cross[0].wait_recv()
                forward[0].start()

            @pl.when(p == 6)
            def _():
                from_cross[1].wait_recv()
                forward[1].start()
            qkv_half(p, near0)
            return carry

        lax.fori_loop(0, N_QKV - 1, near_step, 0)
        wait_ring(N_QKV - 1, NB // 2)
        qkv_last(near0)

        lane = lax.broadcasted_iota(jnp.int32, (HD, T), 0)
        half = jnp.where(lane < HD // 2, lane, lane - HD // 2).astype(F32)
        inv_freq = jnp.exp(half * (-2.0 / HD) * 9.210340371976184)
        ang = pos_v[...].astype(F32) * inv_freq
        cos_t[...] = jnp.cos(ang).T
        sin_t[...] = jnp.where(lane < HD // 2, -jnp.sin(ang), jnp.sin(ang)).T
        acc[...] = jnp.zeros_like(acc)

        forward[0].wait_send()
        norm_piece(cross, 0)
        from_fwd[0].wait_recv()
        norm_piece(diag, 0)
        for i in range(2, NPIECE):
            from_cross[i].wait_recv()
            forward[i].start()
            forward[i - 1].wait_send()
            norm_piece(cross, i - 1)
            from_fwd[i - 1].wait_recv()
            norm_piece(diag, i - 1)
        forward[NPIECE - 1].wait_send()
        norm_piece(cross, NPIECE - 1)
        from_fwd[NPIECE - 1].wait_recv()
        norm_piece(diag, NPIECE - 1)

        def far_step(p, carry):
            qkv_half(p, far0)
            issue(p + RING)
            return carry

        lax.fori_loop(0, N_QKV - 1, far_step, 0)
        qkv_last(far0)
        issue(jnp.int32(N_QKV - 1 + RING))
        for j in range(WORING):
            issue_wo(j)

        def rot(u):
            u = u.astype(F32)
            return (u * cos_t[...] + pltpu.roll(u, HD // 2, 1) * sin_t[...]).astype(BF16)

        def up_step(h, carry):
            g = h + UP0
            s = wait_ring(g)

            @pl.when(h >= 1)
            def _():
                issue(g - 1 + RING)
            qp = 2 + h // 2
            qc = pl.multiple_of(lax.rem(h, 2) * 2 * HD, 2 * HD)
            vp = jnp.where(h < 8, h // 4, N_QKV - 1)
            q = rot(qkv[qp, :, pl.ds(qc, HD)])
            k = rot(qkv[qp, :, pl.ds(qc + HD, HD)])
            first = jnp.dot(m_all[:, pl.ds(0, KC)], ring[s, pl.ds(0, KC), :], preferred_element_type=F32)
            sc = lax.dot_general(q, k, (((1,), (1,)), ((), ())), preferred_element_type=F32) * (HD ** -0.5)
            second = jnp.dot(m_all[:, pl.ds(KC, D - KC)], ring[s, pl.ds(KC, D - KC), :], preferred_element_type=F32)
            mask = lax.broadcasted_iota(jnp.int32, (T, T), 1) <= lax.broadcasted_iota(jnp.int32, (T, T), 0)
            sc = jnp.where(mask, sc, -1e30)
            e = jnp.exp(sc - jnp.max(sc, axis=-1, keepdims=True))
            pr = (e * (1.0 / jnp.sum(e, axis=-1, keepdims=True))).astype(BF16)
            v = qkv[vp, :, pl.ds(pl.multiple_of(lax.rem(h, 4) * HD, HD), HD)]
            ctx[:, cols(h, HD)] = jnp.dot(pr, v, preferred_element_type=F32).astype(BF16)
            gelu_store(jnp.maximum(h - 1, 0))
            acc[...] = first + second
            return carry

        lax.fori_loop(0, N_UP, up_step, 0)

    def back(part):
        def a_copy(j, i):
            blk = partner if i == 0 else diag
            return remote(part.at[j, rows(blk)], ra.at[lax.rem(j, RA), i], a_send.at[j, i], a_recv.at[j, i], partner)

        def b_copy(j):
            return remote(sb.at[j], rb.at[j], b_send.at[j], b_recv.at[j], cross)

        def do_a(j):
            for i in range(2):
                a_copy(j, i).start()

        def do_b(j):
            for i in range(2):
                a_copy(j, i).wait_recv()
            r = lax.rem(j, RA)
            sb[j] = (part[j, rows(cross), :] + ra[r, 1]).astype(BF16)
            b_copy(j).start()
            part[j, rows(t), :] = part[j, rows(t), :] + ra[r, 0]

        def out_copy(j):
            return local(out_v.at[:, cols(j)], out_hbm.at[:, cols(j)], out_sem.at[j])

        def do_c(j):
            b_copy(j).wait_recv()
            out_v[:, cols(j)] = (x_own[:, cols(j)].astype(F32) + (part[j, rows(t), :] + rb[j].astype(F32))).astype(BF16)
            out_copy(j).start()

        def wait_dn(j):
            s = wait_ring(j + DN0)
            w = lax.rem(j, WORING)
            local(wo_hbm.at[:, pl.ds(0, NB)], woring.at[w], wo_sem.at[w]).wait()
            return s, w

        KL = D - NB

        def out_dot(j, s, w):
            return (jnp.dot(abuf[:, pl.ds(0, KL)], ring[s, pl.ds(0, KL), :], preferred_element_type=F32)
                    + jnp.dot(ctx[...], woring[w], preferred_element_type=F32)
                    + jnp.dot(abuf[:, pl.ds(KL, NB)], ring[s, pl.ds(KL, NB), :], preferred_element_type=F32))

        s, w = wait_dn(jnp.int32(0))
        issue(jnp.int32(DN0 - 1 + RING))
        gelu_store(N_UP - 1)
        part[0] = out_dot(0, s, w)

        def dn_step(j, carry):
            g = j + DN0
            s, w = wait_dn(j)
            do_a(j - 1)
            issue(g + RING - 1)

            @pl.when(j + WORING - 1 < N_DN)
            def _():
                issue_wo(j + WORING - 1)

            @pl.when(j >= 2)
            def _():
                do_b(j - 2)

            @pl.when(j >= 4)
            def _():
                do_c(j - 4)
            part[j] = out_dot(j, s, w)
            return carry

        lax.fori_loop(1, N_DN, dn_step, 0)
        do_a(N_DN - 1)
        do_b(N_DN - 2)
        do_c(N_DN - 4)
        do_b(N_DN - 1)
        for j in range(N_DN - 3, N_DN):
            do_c(j)

        def drain(j, carry):
            for i in range(2):
                a_copy(j, i).wait_send()
            b_copy(j).wait_send()
            out_copy(j).wait()
            return carry

        lax.fori_loop(0, N_DN, drain, 0)

    pl.run_scoped(front, pltpu.VMEM((T, D), BF16), pltpu.VMEM((N_QKV, T, NB), BF16),
                  pltpu.VMEM((T, HD), F32), pltpu.VMEM((T, HD), F32))
    pl.run_scoped(back, pltpu.VMEM((N_DN, T, NB), F32))
    for c in to_cross + [to_partner]:
        c.wait_send()


def solution(mesh):
    def local_layer(hidden_blk, attn_gain, attn_bias, mlp_gain, mlp_bias, w_qkv, w_out, w_up, w_down, positions):
        args = (hidden_blk.reshape(TB, D), attn_gain.reshape(1, D), attn_bias.reshape(1, D), mlp_gain.reshape(1, D),
                mlp_bias.reshape(1, D), jnp.transpose(w_qkv, (1, 0, 2)), w_out, w_up, w_down, positions.reshape(1, T))
        dma = pltpu.SemaphoreType.DMA
        out = pl.pallas_call(
            body,
            out_shape=jax.ShapeDtypeStruct((TB, D), BF16),
            in_specs=[pl.BlockSpec(memory_space=pl.ANY)] * 10,
            out_specs=pl.BlockSpec(memory_space=pl.ANY),
            scratch_shapes=[
                pltpu.VMEM((TB, D), BF16),
                pltpu.VMEM((T, D), BF16),
                pltpu.VMEM((T, CTX), BF16),
                pltpu.VMEM((T, NB), F32),
                pltpu.VMEM((4, D), F32),
                pltpu.VMEM((1, T), jnp.int32),
                pltpu.VMEM((RING, D, NB), BF16),
                pltpu.VMEM((WORING, CTX, NB), BF16),
                pltpu.VMEM((RA, 2, TB, NB), F32),
                pltpu.VMEM((N_DN, TB, NB), BF16),
                pltpu.VMEM((N_DN, TB, NB), BF16),
                pltpu.VMEM((TB, D), BF16),
                dma((RING,)), dma((WORING,)), dma((6,)), dma((1,)), dma((1,)), dma((NPIECE,)), dma((NPIECE,)),
                dma((NPIECE,)), dma((NPIECE,)), dma((N_DN, 2)), dma((N_DN, 2)), dma((N_DN,)), dma((N_DN,)), dma((N_DN,)),
            ],
            compiler_params=pltpu.CompilerParams(collective_id=0, has_side_effects=True, vmem_limit_bytes=67043328),
            cost_estimate=pl.CostEstimate(flops=40_300_000_000, bytes_accessed=158_000_000, transcendentals=2_000_000),
            name="layer",
        )(*args)
        return out.reshape(1, TB, D)

    return jax.shard_map(local_layer, mesh=mesh,
                         in_specs=(P('dp', 'tp', None), P(), P(), P(), P(), P(None, 'tp', None), P('tp', None), P(None, 'tp'), P('tp', None), P()),
                         out_specs=P('dp', 'tp', None), check_vma=False)
```

```python
import jax
import jax.numpy as jnp
from jax import lax
from jax.experimental import pallas as pl
from jax.experimental.pallas import tpu as pltpu
from jax.sharding import PartitionSpec as P

MESH = pl.DeviceIdType.MESH
F32 = jnp.float32
BF16 = jnp.bfloat16

D = 5120
T = 256
TB = 64
HD = 128
G = 10
FF = 5120
NB = 512
CTX = G * HD
RING = 9
WORING = 3
SB = 4
N_QKV = 8
N_UP = FF // NB
N_DN = D // NB
UP0 = N_QKV
DN0 = UP0 + N_UP
N_ITEMS = DN0 + N_DN
NPIECE = 4
PROWS = TB // NPIECE
HALF = 2 * TB
RA = 5
KC = 2560


def body(x_hbm, ga_hbm, ba_hbm, gm_hbm, bm_hbm, wqkv_hbm, wo_hbm, wup_hbm, wdn_hbm, pos_hbm,
         out_hbm,
         x_own, abuf, ctx, norms, pos_v,
         ring, woring, ra, sb, rb,
         ring_sem, wo_sem, misc_sem, x_send, x_recv, c_send, c_recv, f_send, f_recv,
         a_send, a_recv, b_send, b_recv, out_sem):
    t = lax.axis_index("tp")
    partner = t + 1 - 2 * lax.rem(t, 2)
    cross = lax.rem(t + 2, 4)
    diag = lax.rem(partner + 2, 4)
    near0 = pl.multiple_of((t // 2) * HALF, HALF)
    far0 = pl.multiple_of((1 - t // 2) * HALF, HALF)

    def local(src, dst, sem):
        return pltpu.make_async_copy(src, dst, sem)

    def remote(src, dst, ssem, rsem, dev):
        return pltpu.make_async_remote_copy(src_ref=src, dst_ref=dst, send_sem=ssem, recv_sem=rsem,
                                            device_id={"tp": dev}, device_id_type=MESH)

    def rows(blk, start=0, n=TB):
        return pl.ds(pl.multiple_of(blk * TB + start, 16), n)

    def cols(i, n=NB):
        return pl.ds(pl.multiple_of(i * n, n), n)

    def issue_qkv(p):
        if p in (0, 1, 7):
            j = {0: 0, 1: 1, 7: 2}[p]
            for h in range(4 if j < 2 else 2):
                local(wqkv_hbm.at[4 * j + h, :, pl.ds(2 * HD, HD)], ring.at[p, :, pl.ds(h * HD, HD)], ring_sem.at[p]).start()
        else:
            for h in range(2):
                local(wqkv_hbm.at[2 * (p - 2) + h, :, pl.ds(0, 2 * HD)], ring.at[p, :, pl.ds(h * 2 * HD, 2 * HD)], ring_sem.at[p]).start()

    def issue(g):
        s = lax.rem(g, RING)

        @pl.when(g < DN0)
        def _():
            local(wup_hbm.at[:, cols(g - UP0)], ring.at[s], ring_sem.at[s]).start()

        @pl.when(jnp.logical_and(g >= DN0, g < N_ITEMS))
        def _():
            local(wdn_hbm.at[:, cols(g - DN0)], ring.at[s], ring_sem.at[s]).start()

    def issue_wo(j, c=None):
        w = lax.rem(j, WORING)
        local(wo_hbm.at[:, cols(j if c is None else c)], woring.at[w], wo_sem.at[w]).start()

    def wait_ring(g, n=NB):
        s = lax.rem(g, RING)
        local(wup_hbm.at[:, pl.ds(0, n)], ring.at[s, :, pl.ds(0, n)], ring_sem.at[s]).wait()
        return s

    xc = local(x_hbm, x_own, misc_sem.at[0])
    xc.start()
    small = [local(h, norms.at[pl.ds(i, 1), :], misc_sem.at[1 + i]) for i, h in enumerate((ga_hbm, ba_hbm, gm_hbm, bm_hbm))]
    small.append(local(pos_hbm, pos_v, misc_sem.at[5]))
    for c in small:
        c.start()
    barrier = pltpu.get_barrier_semaphore()
    for dev in (partner, cross):
        pl.semaphore_signal(barrier, inc=1, device_id={"tp": dev}, device_id_type=MESH)
    for p in range(N_QKV):
        issue_qkv(p)
    issue(jnp.int32(UP0))
    xc.wait()
    pl.semaphore_wait(barrier, 2)

    to_cross = [remote(x_own.at[pl.ds(i * PROWS, PROWS)], abuf.at[rows(t, i * PROWS, PROWS)], c_send.at[i], c_recv.at[i], cross) for i in range(NPIECE)]
    for c in to_cross:
        c.start()
    to_partner = remote(x_own, abuf.at[rows(t)], x_send.at[0], x_recv.at[0], partner)
    to_partner.start()

    def cross_rows(i):
        return abuf.at[rows(cross, i * PROWS, PROWS)]

    def diag_rows(i):
        return abuf.at[rows(diag, i * PROWS, PROWS)]

    from_cross = [remote(cross_rows(i), cross_rows(i), c_send.at[i], c_recv.at[i], cross) for i in range(NPIECE)]
    from_partner = remote(abuf.at[rows(partner)], abuf.at[rows(partner)], x_send.at[0], x_recv.at[0], partner)
    forward = [remote(cross_rows(i), cross_rows(i), f_send.at[i], f_recv.at[i], partner) for i in range(NPIECE)]
    from_fwd = [remote(diag_rows(i), diag_rows(i), f_send.at[i], f_recv.at[i], partner) for i in range(NPIECE)]

    def gelu_store(u, j):
        abuf[:, cols(j)] = (0.5 * u * (1.0 + lax.erf(u * 0.7071067811865476))).astype(BF16)

    def front(m_all, qkv, cos_t, sin_t, acc):
        LR = 16

        def norm_rows(src, r_src, r_dst):
            xr = src[r_src, :].astype(F32)
            mean = jnp.mean(xr, axis=-1, keepdims=True)
            cen = xr - mean
            var = jnp.mean(cen * cen, axis=-1, keepdims=True)
            z = cen * lax.rsqrt(var + 1e-5)
            abuf[r_dst, :] = (z * norms[0:1, :] + norms[1:2, :]).astype(BF16)
            m_all[r_dst, :] = (z * norms[2:3, :] + norms[3:4, :]).astype(BF16)

        for c in small:
            c.wait()

        def own_step(i, carry):
            norm_rows(x_own, pl.ds(pl.multiple_of(i * LR, LR), LR), rows(t, i * LR, LR))
            return carry

        lax.fori_loop(0, TB // LR, own_step, 0)
        from_partner.wait_recv()

        def blk_step(i, carry):
            r = rows(partner, i * LR, LR)
            norm_rows(abuf, r, r)
            return carry

        lax.fori_loop(0, TB // LR, blk_step, 0)

        def norm_piece(blk, i):
            r = rows(blk, i * PROWS, PROWS)
            norm_rows(abuf, r, r)

        def qkv_half(p, r0):
            r = pl.ds(r0, HALF)
            qkv[p, r, :] = jnp.dot(abuf[r, :], ring[p], preferred_element_type=F32).astype(BF16)

        def qkv_last(r0):
            r = pl.ds(r0, HALF)
            p = N_QKV - 1
            n = NB // 2
            qkv[p, r, pl.ds(0, n)] = jnp.dot(abuf[r, :], ring[p, :, pl.ds(0, n)], preferred_element_type=F32).astype(BF16)

        def near_step(p, carry):
            wait_ring(p)

            @pl.when(p == 3)
            def _():
                from_cross[0].wait_recv()
                forward[0].start()

            @pl.when(p == 6)
            def _():
                from_cross[1].wait_recv()
                forward[1].start()
            qkv_half(p, near0)
            return carry

        lax.fori_loop(0, N_QKV - 1, near_step, 0)
        wait_ring(N_QKV - 1, NB // 2)
        qkv_last(near0)

        lane = lax.broadcasted_iota(jnp.int32, (HD, T), 0)
        half = jnp.where(lane < HD // 2, lane, lane - HD // 2).astype(F32)
        inv_freq = jnp.exp(half * (-2.0 / HD) * 9.210340371976184)
        ang = pos_v[...].astype(F32) * inv_freq
        cos_t[...] = jnp.cos(ang).T
        sin_t[...] = jnp.where(lane < HD // 2, -jnp.sin(ang), jnp.sin(ang)).T
        acc[...] = jnp.zeros_like(acc)

        forward[0].wait_send()
        norm_piece(cross, 0)
        from_fwd[0].wait_recv()
        norm_piece(diag, 0)
        for i in range(2, NPIECE):
            from_cross[i].wait_recv()
            forward[i].start()
            forward[i - 1].wait_send()
            norm_piece(cross, i - 1)
            from_fwd[i - 1].wait_recv()
            norm_piece(diag, i - 1)
        forward[NPIECE - 1].wait_send()
        norm_piece(cross, NPIECE - 1)
        from_fwd[NPIECE - 1].wait_recv()
        norm_piece(diag, NPIECE - 1)

        def far_step(i, carry):
            for p in (2 * i, 2 * i + 1):
                qkv_half(p, far0)
            for p in (2 * i, 2 * i + 1):
                issue(p + RING)
            return carry

        lax.fori_loop(0, N_QKV // 2 - 1, far_step, 0)
        qkv_half(N_QKV - 2, far0)
        qkv_last(far0)
        for p in (N_QKV - 2, N_QKV - 1):
            issue(jnp.int32(p + RING))
        for j in range(WORING):
            issue_wo(j)

        def rot(u):
            u = u.astype(F32)
            return (u * cos_t[...] + pltpu.roll(u, HD // 2, 1) * sin_t[...]).astype(BF16)

        def head(h, dot_a, dot_b):
            qp = 2 + h // 2
            qc = pl.multiple_of(lax.rem(h, 2) * 2 * HD, 2 * HD)
            vp = jnp.where(h < 8, h // 4, N_QKV - 1)
            q = rot(qkv[qp, :, pl.ds(qc, HD)])
            k = rot(qkv[qp, :, pl.ds(qc + HD, HD)])
            first = dot_a()
            sc = lax.dot_general(q, k, (((1,), (1,)), ((), ())), preferred_element_type=F32) * (HD ** -0.5)
            second = dot_b()
            mask = lax.broadcasted_iota(jnp.int32, (T, T), 1) <= lax.broadcasted_iota(jnp.int32, (T, T), 0)
            sc = jnp.where(mask, sc, -1e30)
            e = jnp.exp(sc - jnp.max(sc, axis=-1, keepdims=True))
            pr = (e * (1.0 / jnp.sum(e, axis=-1, keepdims=True))).astype(BF16)
            v = qkv[vp, :, pl.ds(pl.multiple_of(lax.rem(h, 4) * HD, HD), HD)]
            ctx[:, cols(h, HD)] = jnp.dot(pr, v, preferred_element_type=F32).astype(BF16)
            return first + second

        def up_step(i, carry):
            h0 = 2 * i
            g0 = h0 + UP0
            ss = [wait_ring(g0), wait_ring(g0 + 1)]

            @pl.when(i >= 1)
            def _():
                issue(g0 - 2 + RING)
                issue(g0 - 1 + RING)

            def part_dot(s, lo):
                r = pl.ds(lo, KC)
                return lambda: jnp.dot(m_all[:, r], ring[s, r, :], preferred_element_type=F32)
            gelu_store(acc[...], jnp.maximum(h0 - 1, 0))
            u0 = head(h0, part_dot(ss[0], 0), part_dot(ss[0], KC))
            gelu_store(u0, h0)
            u1 = head(h0 + 1, part_dot(ss[1], 0), part_dot(ss[1], KC))
            acc[...] = u1
            return carry

        lax.fori_loop(0, N_UP // 2, up_step, 0)
        gelu_store(acc[...], N_UP - 1)

    def back(part):
        def a_copy(j, i):
            blk = partner if i == 0 else diag
            return remote(part.at[j, rows(blk)], ra.at[lax.rem(j, RA), i], a_send.at[j, i], a_recv.at[j, i], partner)

        def b_copy(j):
            return remote(sb.at[lax.rem(j, SB)], rb.at[j], b_send.at[j], b_recv.at[j], cross)

        def do_a(j):
            for i in range(2):
                a_copy(j, i).start()

        def do_b(j):
            for i in range(2):
                a_copy(j, i).wait_recv()
            r = lax.rem(j, RA)

            @pl.when(j >= SB)
            def _():
                b_copy(j - SB).wait_send()
            sb[lax.rem(j, SB)] = (part[j, rows(cross), :] + ra[r, 1]).astype(BF16)
            b_copy(j).start()
            part[j, rows(t), :] = part[j, rows(t), :] + ra[r, 0]

        def out_copy(j):
            return local(x_own.at[:, cols(j)], out_hbm.at[:, cols(j)], out_sem.at[j])

        def do_c(j):
            b_copy(j).wait_recv()
            x_own[:, cols(j)] = (x_own[:, cols(j)].astype(F32) + (part[j, rows(t), :] + rb[j].astype(F32))).astype(BF16)
            out_copy(j).start()

        def wait_dn(j):
            s = wait_ring(j + DN0)
            w = lax.rem(j, WORING)
            local(wo_hbm.at[:, pl.ds(0, NB)], woring.at[w], wo_sem.at[w]).wait()
            return s, w

        def out_dot(s, w):
            return (jnp.dot(ctx[...], woring[w], preferred_element_type=F32)
                    + jnp.dot(abuf[...], ring[s], preferred_element_type=F32))

        def refill(j):
            @pl.when(j + DN0 + RING < N_ITEMS)
            def _():
                issue(j + DN0 + RING)

        for g in (DN0 - 2, DN0 - 1):
            issue(jnp.int32(g + RING))

        def dn_pair(i, carry):
            j = 2 * i
            s0, w0 = wait_dn(j)
            s1, w1 = wait_dn(j + 1)

            @pl.when(i >= 1)
            def _():
                do_a(j - 1)
                refill(j - 2)
                refill(j - 1)
                issue_wo(j + 2, jnp.minimum(j + 2, N_DN - 1))
                do_b(j - 2)

            @pl.when(i >= 2)
            def _():
                do_b(j - 3)

            @pl.when(i >= 3)
            def _():
                do_c(j - 6)
                do_c(j - 5)
            part[j] = out_dot(s0, w0)
            issue_wo(j + 3, jnp.minimum(j + 3, N_DN - 1))
            part[j + 1] = out_dot(s1, w1)
            do_a(j)
            return carry

        N_PAIR = 5
        lax.fori_loop(0, N_PAIR, dn_pair, 0)
        do_a(N_DN - 1)
        do_b(N_DN - 3)
        do_b(N_DN - 2)
        do_c(4)
        do_c(5)
        do_b(N_DN - 1)
        for j in range(6, N_DN):
            do_c(j)

        for j in (N_DN, N_DN + 1):
            local(wo_hbm.at[:, pl.ds(0, NB)], woring.at[j % WORING], wo_sem.at[j % WORING]).wait()
        for j in range(N_DN - SB, N_DN):
            b_copy(j).wait_send()

        def drain(j, carry):
            for i in range(2):
                a_copy(j, i).wait_send()
            out_copy(j).wait()
            return carry

        lax.fori_loop(0, N_DN, drain, 0)

    pl.run_scoped(front, pltpu.VMEM((T, D), BF16), pltpu.VMEM((N_QKV, T, NB), BF16),
                  pltpu.VMEM((T, HD), F32), pltpu.VMEM((T, HD), F32), pltpu.VMEM((T, NB), F32))
    for c in to_cross + [to_partner]:
        c.wait_send()
    pl.run_scoped(back, pltpu.VMEM((N_DN, T, NB), F32))


def solution(mesh):
    def local_layer(hidden_blk, attn_gain, attn_bias, mlp_gain, mlp_bias, w_qkv, w_out, w_up, w_down, positions):
        args = (hidden_blk.reshape(TB, D), attn_gain.reshape(1, D), attn_bias.reshape(1, D), mlp_gain.reshape(1, D),
                mlp_bias.reshape(1, D), jnp.transpose(w_qkv, (1, 0, 2)), w_out, w_up, w_down, positions.reshape(1, T))
        dma = pltpu.SemaphoreType.DMA
        out = pl.pallas_call(
            body,
            out_shape=jax.ShapeDtypeStruct((TB, D), BF16),
            in_specs=[pl.BlockSpec(memory_space=pl.ANY)] * 10,
            out_specs=pl.BlockSpec(memory_space=pl.ANY),
            scratch_shapes=[
                pltpu.VMEM((TB, D), BF16),
                pltpu.VMEM((T, D), BF16),
                pltpu.VMEM((T, CTX), BF16),
                pltpu.VMEM((4, D), F32),
                pltpu.VMEM((1, T), jnp.int32),
                pltpu.VMEM((RING, D, NB), BF16),
                pltpu.VMEM((WORING, CTX, NB), BF16),
                pltpu.VMEM((RA, 2, TB, NB), F32),
                pltpu.VMEM((SB, TB, NB), BF16),
                pltpu.VMEM((N_DN, TB, NB), BF16),
                dma((RING,)), dma((WORING,)), dma((6,)), dma((1,)), dma((1,)), dma((NPIECE,)), dma((NPIECE,)),
                dma((NPIECE,)), dma((NPIECE,)), dma((N_DN, 2)), dma((N_DN, 2)), dma((N_DN,)), dma((N_DN,)), dma((N_DN,)),
            ],
            compiler_params=pltpu.CompilerParams(collective_id=0, has_side_effects=True, vmem_limit_bytes=67043328),
            cost_estimate=pl.CostEstimate(flops=40_300_000_000, bytes_accessed=158_000_000, transcendentals=2_000_000),
            name="layer",
        )(*args)
        return out.reshape(1, TB, D)

    return jax.shard_map(local_layer, mesh=mesh,
                         in_specs=(P('dp', 'tp', None), P(), P(), P(), P(), P(None, 'tp', None), P('tp', None), P(None, 'tp'), P('tp', None), P()),
                         out_specs=P('dp', 'tp', None), check_vma=False)
```

```python
import jax
import jax.numpy as jnp
from jax import lax
from jax.experimental import pallas as pl
from jax.experimental.pallas import tpu as pltpu
from jax.sharding import PartitionSpec as P

MESH = pl.DeviceIdType.MESH
F32 = jnp.float32
BF16 = jnp.bfloat16

D = 5120
T = 256
TB = 64
HD = 128
G = 10
FF = 5120
NB = 512
CTX = G * HD
RING = 9
WORING = 3
SB = 4
N_QKV = 8
N_UP = FF // NB
N_DN = D // NB
UP0 = N_QKV
DN0 = UP0 + N_UP
N_ITEMS = DN0 + N_DN
NPIECE = 4
PROWS = TB // NPIECE
HALF = 2 * TB
RA = 5
KC = 2560


def body(x_hbm, ga_hbm, ba_hbm, gm_hbm, bm_hbm, wqkv_hbm, wo_hbm, wup_hbm, wdn_hbm, pos_hbm,
         out_hbm,
         x_own, abuf, ctx, norms, pos_v,
         ring, woring, ra, sb, rb,
         ring_sem, wo_sem, misc_sem, x_send, x_recv, c_send, c_recv, f_send, f_recv,
         a_send, a_recv, b_send, b_recv, out_sem):
    t = lax.axis_index("tp")
    partner = t + 1 - 2 * lax.rem(t, 2)
    cross = lax.rem(t + 2, 4)
    diag = lax.rem(partner + 2, 4)
    near0 = pl.multiple_of((t // 2) * HALF, HALF)
    far0 = pl.multiple_of((1 - t // 2) * HALF, HALF)

    def local(src, dst, sem):
        return pltpu.make_async_copy(src, dst, sem)

    def remote(src, dst, ssem, rsem, dev):
        return pltpu.make_async_remote_copy(src_ref=src, dst_ref=dst, send_sem=ssem, recv_sem=rsem,
                                            device_id={"tp": dev}, device_id_type=MESH)

    def rows(blk, start=0, n=TB):
        return pl.ds(pl.multiple_of(blk * TB + start, 16), n)

    def cols(i, n=NB):
        return pl.ds(pl.multiple_of(i * n, n), n)

    def issue_qkv(p):
        if p in (0, 1, 7):
            j = {0: 0, 1: 1, 7: 2}[p]
            for h in range(4 if j < 2 else 2):
                local(wqkv_hbm.at[4 * j + h, :, pl.ds(2 * HD, HD)], ring.at[p, :, pl.ds(h * HD, HD)], ring_sem.at[p]).start()
        else:
            for h in range(2):
                local(wqkv_hbm.at[2 * (p - 2) + h, :, pl.ds(0, 2 * HD)], ring.at[p, :, pl.ds(h * 2 * HD, 2 * HD)], ring_sem.at[p]).start()

    def issue(g):
        s = lax.rem(g, RING)

        @pl.when(g < DN0)
        def _():
            local(wup_hbm.at[:, cols(g - UP0)], ring.at[s], ring_sem.at[s]).start()

        @pl.when(jnp.logical_and(g >= DN0, g < N_ITEMS))
        def _():
            local(wdn_hbm.at[:, cols(g - DN0)], ring.at[s], ring_sem.at[s]).start()

    def issue_wo(j):
        w = lax.rem(j, WORING)
        local(wo_hbm.at[:, cols(j)], woring.at[w], wo_sem.at[w]).start()

    def wait_ring(g, n=NB):
        s = lax.rem(g, RING)
        local(wup_hbm.at[:, pl.ds(0, n)], ring.at[s, :, pl.ds(0, n)], ring_sem.at[s]).wait()
        return s

    xc = local(x_hbm, x_own, misc_sem.at[0])
    xc.start()
    small = [local(h, norms.at[pl.ds(i, 1), :], misc_sem.at[1 + i]) for i, h in enumerate((ga_hbm, ba_hbm, gm_hbm, bm_hbm))]
    small.append(local(pos_hbm, pos_v, misc_sem.at[5]))
    for c in small:
        c.start()
    barrier = pltpu.get_barrier_semaphore()
    for dev in (partner, cross):
        pl.semaphore_signal(barrier, inc=1, device_id={"tp": dev}, device_id_type=MESH)
    for p in range(N_QKV):
        issue_qkv(p)
    issue(jnp.int32(UP0))
    xc.wait()
    pl.semaphore_wait(barrier, 2)

    to_cross = [remote(x_own.at[pl.ds(i * PROWS, PROWS)], abuf.at[rows(t, i * PROWS, PROWS)], c_send.at[i], c_recv.at[i], cross) for i in range(NPIECE)]
    for c in to_cross:
        c.start()
    to_partner = remote(x_own, abuf.at[rows(t)], x_send.at[0], x_recv.at[0], partner)
    to_partner.start()

    def cross_rows(i):
        return abuf.at[rows(cross, i * PROWS, PROWS)]

    def diag_rows(i):
        return abuf.at[rows(diag, i * PROWS, PROWS)]

    from_cross = [remote(cross_rows(i), cross_rows(i), c_send.at[i], c_recv.at[i], cross) for i in range(NPIECE)]
    from_partner = remote(abuf.at[rows(partner)], abuf.at[rows(partner)], x_send.at[0], x_recv.at[0], partner)
    forward = [remote(cross_rows(i), cross_rows(i), f_send.at[i], f_recv.at[i], partner) for i in range(NPIECE)]
    from_fwd = [remote(diag_rows(i), diag_rows(i), f_send.at[i], f_recv.at[i], partner) for i in range(NPIECE)]

    def gelu_store(u, j):
        abuf[:, cols(j)] = (0.5 * u * (1.0 + lax.erf(u * 0.7071067811865476))).astype(BF16)

    def front(m_all, qkv, cos_t, sin_t, acc):
        LR = 16

        def norm_rows(src, r_src, r_dst):
            xr = src[r_src, :].astype(F32)
            mean = jnp.mean(xr, axis=-1, keepdims=True)
            cen = xr - mean
            var = jnp.mean(cen * cen, axis=-1, keepdims=True)
            z = cen * lax.rsqrt(var + 1e-5)
            abuf[r_dst, :] = (z * norms[0:1, :] + norms[1:2, :]).astype(BF16)
            m_all[r_dst, :] = (z * norms[2:3, :] + norms[3:4, :]).astype(BF16)

        for c in small:
            c.wait()

        def own_step(i, carry):
            norm_rows(x_own, pl.ds(pl.multiple_of(i * LR, LR), LR), rows(t, i * LR, LR))
            return carry

        lax.fori_loop(0, TB // LR, own_step, 0)
        from_partner.wait_recv()

        def blk_step(i, carry):
            r = rows(partner, i * LR, LR)
            norm_rows(abuf, r, r)
            return carry

        lax.fori_loop(0, TB // LR, blk_step, 0)

        def norm_piece(blk, i):
            r = rows(blk, i * PROWS, PROWS)
            norm_rows(abuf, r, r)

        def qkv_half(p, r0):
            r = pl.ds(r0, HALF)
            qkv[p, r, :] = jnp.dot(abuf[r, :], ring[p], preferred_element_type=F32).astype(BF16)

        def qkv_last(r0):
            r = pl.ds(r0, HALF)
            p = N_QKV - 1
            n = NB // 2
            qkv[p, r, pl.ds(0, n)] = jnp.dot(abuf[r, :], ring[p, :, pl.ds(0, n)], preferred_element_type=F32).astype(BF16)

        def near_step(p, carry):
            wait_ring(p)

            @pl.when(p == 3)
            def _():
                from_cross[0].wait_recv()
                forward[0].start()

            @pl.when(p == 6)
            def _():
                from_cross[1].wait_recv()
                forward[1].start()
            qkv_half(p, near0)
            return carry

        lax.fori_loop(0, N_QKV - 1, near_step, 0)
        wait_ring(N_QKV - 1, NB // 2)
        qkv_last(near0)

        lane = lax.broadcasted_iota(jnp.int32, (HD, T), 0)
        half = jnp.where(lane < HD // 2, lane, lane - HD // 2).astype(F32)
        inv_freq = jnp.exp(half * (-2.0 / HD) * 9.210340371976184)
        ang = pos_v[...].astype(F32) * inv_freq
        cos_t[...] = jnp.cos(ang).T
        sin_t[...] = jnp.where(lane < HD // 2, -jnp.sin(ang), jnp.sin(ang)).T
        acc[...] = jnp.zeros_like(acc)

        forward[0].wait_send()
        norm_piece(cross, 0)
        from_fwd[0].wait_recv()
        norm_piece(diag, 0)
        for i in range(2, NPIECE):
            from_cross[i].wait_recv()
            forward[i].start()
            forward[i - 1].wait_send()
            norm_piece(cross, i - 1)
            from_fwd[i - 1].wait_recv()
            norm_piece(diag, i - 1)
        forward[NPIECE - 1].wait_send()
        norm_piece(cross, NPIECE - 1)
        from_fwd[NPIECE - 1].wait_recv()
        norm_piece(diag, NPIECE - 1)

        def far_step(i, carry):
            for p in (2 * i, 2 * i + 1):
                qkv_half(p, far0)
            for p in (2 * i, 2 * i + 1):
                issue(p + RING)
            return carry

        lax.fori_loop(0, N_QKV // 2 - 1, far_step, 0)
        qkv_half(N_QKV - 2, far0)
        qkv_last(far0)
        for p in (N_QKV - 2, N_QKV - 1):
            issue(jnp.int32(p + RING))
        for j in range(WORING):
            issue_wo(j)

        def rot(u):
            u = u.astype(F32)
            return (u * cos_t[...] + pltpu.roll(u, HD // 2, 1) * sin_t[...]).astype(BF16)

        def head(h, dot_a, dot_b):
            qp = 2 + h // 2
            qc = pl.multiple_of(lax.rem(h, 2) * 2 * HD, 2 * HD)
            vp = jnp.where(h < 8, h // 4, N_QKV - 1)
            q = rot(qkv[qp, :, pl.ds(qc, HD)])
            k = rot(qkv[qp, :, pl.ds(qc + HD, HD)])
            first = dot_a()
            sc = lax.dot_general(q, k, (((1,), (1,)), ((), ())), preferred_element_type=F32) * (HD ** -0.5)
            second = dot_b()
            mask = lax.broadcasted_iota(jnp.int32, (T, T), 1) <= lax.broadcasted_iota(jnp.int32, (T, T), 0)
            sc = jnp.where(mask, sc, -1e30)
            e = jnp.exp(sc - jnp.max(sc, axis=-1, keepdims=True))
            pr = (e * (1.0 / jnp.sum(e, axis=-1, keepdims=True))).astype(BF16)
            v = qkv[vp, :, pl.ds(pl.multiple_of(lax.rem(h, 4) * HD, HD), HD)]
            ctx[:, cols(h, HD)] = jnp.dot(pr, v, preferred_element_type=F32).astype(BF16)
            return first + second

        def up_step(i, carry):
            h0 = 2 * i
            g0 = h0 + UP0
            ss = [wait_ring(g0), wait_ring(g0 + 1)]

            @pl.when(i >= 1)
            def _():
                issue(g0 - 2 + RING)
                issue(g0 - 1 + RING)

            def part_dot(s, lo):
                r = pl.ds(lo, KC)
                return lambda: jnp.dot(m_all[:, r], ring[s, r, :], preferred_element_type=F32)
            gelu_store(acc[...], jnp.maximum(h0 - 1, 0))
            u0 = head(h0, part_dot(ss[0], 0), part_dot(ss[0], KC))
            gelu_store(u0, h0)
            u1 = head(h0 + 1, part_dot(ss[1], 0), part_dot(ss[1], KC))
            acc[...] = u1
            return carry

        lax.fori_loop(0, N_UP // 2, up_step, 0)
        gelu_store(acc[...], N_UP - 1)

    def back(part):
        def a_copy(j, i):
            blk = partner if i == 0 else diag
            return remote(part.at[j, rows(blk)], ra.at[lax.rem(j, RA), i], a_send.at[j, i], a_recv.at[j, i], partner)

        def b_copy(j):
            return remote(sb.at[lax.rem(j, SB)], rb.at[j], b_send.at[j], b_recv.at[j], cross)

        def do_a(j):
            for i in range(2):
                a_copy(j, i).start()

        def do_b(j):
            for i in range(2):
                a_copy(j, i).wait_recv()
            r = lax.rem(j, RA)

            @pl.when(j >= SB)
            def _():
                b_copy(j - SB).wait_send()
            sb[lax.rem(j, SB)] = (part[j, rows(cross), :] + ra[r, 1]).astype(BF16)
            b_copy(j).start()
            part[j, rows(t), :] = part[j, rows(t), :] + ra[r, 0]

        def out_copy(j):
            return local(x_own.at[:, cols(j)], out_hbm.at[:, cols(j)], out_sem.at[j])

        def do_c(j):
            b_copy(j).wait_recv()
            x_own[:, cols(j)] = (x_own[:, cols(j)].astype(F32) + (part[j, rows(t), :] + rb[j].astype(F32))).astype(BF16)
            out_copy(j).start()

        def wait_dn(j):
            s = wait_ring(j + DN0)
            w = lax.rem(j, WORING)
            local(wo_hbm.at[:, pl.ds(0, NB)], woring.at[w], wo_sem.at[w]).wait()
            return s, w

        def out_dot(s, w):
            return (jnp.dot(ctx[...], woring[w], preferred_element_type=F32)
                    + jnp.dot(abuf[...], ring[s], preferred_element_type=F32))

        def refill(j):
            @pl.when(j + DN0 + RING < N_ITEMS)
            def _():
                issue(j + DN0 + RING)

        for g in (DN0 - 2, DN0 - 1):
            issue(jnp.int32(g + RING))

        def dn_pair(i, carry):
            j = 2 * i
            s0, w0 = wait_dn(j)
            s1, w1 = wait_dn(j + 1)

            @pl.when(i >= 1)
            def _():
                do_a(j - 1)
                refill(j - 2)
                refill(j - 1)
                issue_wo(j + 2)

            @pl.when(i >= 2)
            def _():
                do_b(j - 3)

            @pl.when(i >= 1)
            def _():
                do_b(j - 2)

            @pl.when(i >= 4)
            def _():
                do_c(j - 7)

            @pl.when(i >= 3)
            def _():
                do_c(j - 6)
            part[j] = out_dot(s0, w0)
            lo, hi = pl.ds(0, KC), pl.ds(KC, FF - KC)
            first = (jnp.dot(ctx[...], woring[w1], preferred_element_type=F32)
                     + jnp.dot(abuf[:, lo], ring[s1, lo, :], preferred_element_type=F32))
            issue_wo(j + 3)
            do_a(j)
            part[j + 1] = first + jnp.dot(abuf[:, hi], ring[s1, hi, :], preferred_element_type=F32)
            return carry

        lax.fori_loop(0, N_DN // 2 - 1, dn_pair, 0)
        s, w = wait_dn(N_DN - 2)
        do_a(7)
        do_b(5)
        do_b(6)
        do_c(1)
        part[8] = out_dot(s, w)
        s, w = wait_dn(N_DN - 1)
        do_a(8)
        do_b(7)
        do_c(2)
        do_c(3)
        part[9] = out_dot(s, w)
        do_a(9)
        do_b(8)
        do_c(4)
        do_c(5)
        do_c(6)
        do_b(9)
        do_c(7)
        do_c(8)
        do_c(9)

        for j in range(N_DN - SB, N_DN):
            b_copy(j).wait_send()

        def drain(j, carry):
            for i in range(2):
                a_copy(j, i).wait_send()
            out_copy(j).wait()
            return carry

        lax.fori_loop(0, N_DN, drain, 0)

    pl.run_scoped(front, pltpu.VMEM((T, D), BF16), pltpu.VMEM((N_QKV, T, NB), BF16),
                  pltpu.VMEM((T, HD), F32), pltpu.VMEM((T, HD), F32), pltpu.VMEM((T, NB), F32))
    for c in to_cross + [to_partner]:
        c.wait_send()
    pl.run_scoped(back, pltpu.VMEM((N_DN, T, NB), F32))


def solution(mesh):
    def local_layer(hidden_blk, attn_gain, attn_bias, mlp_gain, mlp_bias, w_qkv, w_out, w_up, w_down, positions):
        args = (hidden_blk.reshape(TB, D), attn_gain.reshape(1, D), attn_bias.reshape(1, D), mlp_gain.reshape(1, D),
                mlp_bias.reshape(1, D), jnp.transpose(w_qkv, (1, 0, 2)), w_out, w_up, w_down, positions.reshape(1, T))
        dma = pltpu.SemaphoreType.DMA
        out = pl.pallas_call(
            body,
            out_shape=jax.ShapeDtypeStruct((TB, D), BF16),
            in_specs=[pl.BlockSpec(memory_space=pl.ANY)] * 10,
            out_specs=pl.BlockSpec(memory_space=pl.ANY),
            scratch_shapes=[
                pltpu.VMEM((TB, D), BF16),
                pltpu.VMEM((T, D), BF16),
                pltpu.VMEM((T, CTX), BF16),
                pltpu.VMEM((4, D), F32),
                pltpu.VMEM((1, T), jnp.int32),
                pltpu.VMEM((RING, D, NB), BF16),
                pltpu.VMEM((WORING, CTX, NB), BF16),
                pltpu.VMEM((RA, 2, TB, NB), F32),
                pltpu.VMEM((SB, TB, NB), BF16),
                pltpu.VMEM((N_DN, TB, NB), BF16),
                dma((RING,)), dma((WORING,)), dma((6,)), dma((1,)), dma((1,)), dma((NPIECE,)), dma((NPIECE,)),
                dma((NPIECE,)), dma((NPIECE,)), dma((N_DN, 2)), dma((N_DN, 2)), dma((N_DN,)), dma((N_DN,)), dma((N_DN,)),
            ],
            compiler_params=pltpu.CompilerParams(collective_id=0, has_side_effects=True, vmem_limit_bytes=67043328),
            cost_estimate=pl.CostEstimate(flops=40_300_000_000, bytes_accessed=158_000_000, transcendentals=2_000_000),
            name="layer",
        )(*args)
        return out.reshape(1, TB, D)

    return jax.shard_map(local_layer, mesh=mesh,
                         in_specs=(P('dp', 'tp', None), P(), P(), P(), P(), P(None, 'tp', None), P('tp', None), P(None, 'tp'), P('tp', None), P()),
                         out_specs=P('dp', 'tp', None), check_vma=False)
```

```python
import jax
import jax.numpy as jnp
from jax import lax
from jax.experimental import pallas as pl
from jax.experimental.pallas import tpu as pltpu
from jax.sharding import PartitionSpec as P

MESH = pl.DeviceIdType.MESH
F32 = jnp.float32
BF16 = jnp.bfloat16

D = 5120
T = 256
TB = 64
HD = 128
G = 10
FF = 5120
NB = 512
CTX = G * HD
RING = 9
SB = 4
N_QKV = 8
N_UP = FF // NB
N_DN = D // NB
UP0 = N_QKV
WO0 = UP0 + N_UP
N_WO = 3
DN0 = WO0 + N_WO
N_ITEMS = DN0 + N_DN
NPIECE = 4
PROWS = TB // NPIECE
HALF = 2 * TB
RA = 5
KC = 2560


def body(x_hbm, ga_hbm, ba_hbm, gm_hbm, bm_hbm, wqkv_hbm, wo_hbm, wup_hbm, wdn_hbm, pos_hbm,
         out_hbm,
         x_own, abuf, ctx, norms, pos_v,
         ring, ra, sb, rb,
         ring_sem, misc_sem, x_send, x_recv, c_send, c_recv, f_send, f_recv,
         a_send, a_recv, b_send, b_recv, out_sem):
    t = lax.axis_index("tp")
    partner = t + 1 - 2 * lax.rem(t, 2)
    cross = lax.rem(t + 2, 4)
    diag = lax.rem(partner + 2, 4)
    near0 = pl.multiple_of((t // 2) * HALF, HALF)
    far0 = pl.multiple_of((1 - t // 2) * HALF, HALF)

    def local(src, dst, sem):
        return pltpu.make_async_copy(src, dst, sem)

    def remote(src, dst, ssem, rsem, dev):
        return pltpu.make_async_remote_copy(src_ref=src, dst_ref=dst, send_sem=ssem, recv_sem=rsem,
                                            device_id={"tp": dev}, device_id_type=MESH)

    def rows(blk, start=0, n=TB):
        return pl.ds(pl.multiple_of(blk * TB + start, 16), n)

    def cols(i, n=NB):
        return pl.ds(pl.multiple_of(i * n, n), n)

    def issue_qkv(p):
        if p in (0, 1, 7):
            j = {0: 0, 1: 1, 7: 2}[p]
            for h in range(4 if j < 2 else 2):
                local(wqkv_hbm.at[4 * j + h, :, pl.ds(2 * HD, HD)], ring.at[p, :, pl.ds(h * HD, HD)], ring_sem.at[p]).start()
        else:
            for h in range(2):
                local(wqkv_hbm.at[2 * (p - 2) + h, :, pl.ds(0, 2 * HD)], ring.at[p, :, pl.ds(h * 2 * HD, 2 * HD)], ring_sem.at[p]).start()

    def issue(g):
        s = lax.rem(g, RING)

        @pl.when(g < WO0)
        def _():
            local(wup_hbm.at[:, cols(g - UP0)], ring.at[s], ring_sem.at[s]).start()

        for q in range(N_WO):
            @pl.when(g == WO0 + q)
            def _(q=q):
                for h in range(4 if q < 2 else 2):
                    local(wo_hbm.at[:, pl.ds((4 * q + h) * NB, NB)], ring.at[(WO0 + q) % RING, pl.ds(h * CTX, CTX), :],
                          ring_sem.at[(WO0 + q) % RING]).start()

        @pl.when(jnp.logical_and(g >= DN0, g < N_ITEMS))
        def _():
            local(wdn_hbm.at[:, cols(g - DN0)], ring.at[s], ring_sem.at[s]).start()

    def wait_ring(g, n=NB):
        s = lax.rem(g, RING)
        local(wup_hbm.at[:, pl.ds(0, n)], ring.at[s, :, pl.ds(0, n)], ring_sem.at[s]).wait()
        return s

    xc = local(x_hbm, x_own, misc_sem.at[0])
    xc.start()
    small = [local(h, norms.at[pl.ds(i, 1), :], misc_sem.at[1 + i]) for i, h in enumerate((ga_hbm, ba_hbm, gm_hbm, bm_hbm))]
    small.append(local(pos_hbm, pos_v, misc_sem.at[5]))
    for c in small:
        c.start()
    barrier = pltpu.get_barrier_semaphore()
    for dev in (partner, cross):
        pl.semaphore_signal(barrier, inc=1, device_id={"tp": dev}, device_id_type=MESH)
    for p in range(N_QKV):
        issue_qkv(p)
    issue(jnp.int32(UP0))
    xc.wait()
    pl.semaphore_wait(barrier, 2)

    to_cross = [remote(x_own.at[pl.ds(i * PROWS, PROWS)], abuf.at[rows(t, i * PROWS, PROWS)], c_send.at[i], c_recv.at[i], cross) for i in range(NPIECE)]
    for c in to_cross:
        c.start()
    to_partner = remote(x_own, abuf.at[rows(t)], x_send.at[0], x_recv.at[0], partner)
    to_partner.start()

    def cross_rows(i):
        return abuf.at[rows(cross, i * PROWS, PROWS)]

    def diag_rows(i):
        return abuf.at[rows(diag, i * PROWS, PROWS)]

    from_cross = [remote(cross_rows(i), cross_rows(i), c_send.at[i], c_recv.at[i], cross) for i in range(NPIECE)]
    from_partner = remote(abuf.at[rows(partner)], abuf.at[rows(partner)], x_send.at[0], x_recv.at[0], partner)
    forward = [remote(cross_rows(i), cross_rows(i), f_send.at[i], f_recv.at[i], partner) for i in range(NPIECE)]
    from_fwd = [remote(diag_rows(i), diag_rows(i), f_send.at[i], f_recv.at[i], partner) for i in range(NPIECE)]

    def gelu_store(u, j):
        abuf[:, cols(j)] = (0.5 * u * (1.0 + lax.erf(u * 0.7071067811865476))).astype(BF16)

    def front(m_all, qkv, cos_t, sin_t, acc):
        LR = 16

        def norm_rows(src, r_src, r_dst):
            xr = src[r_src, :].astype(F32)
            mean = jnp.mean(xr, axis=-1, keepdims=True)
            cen = xr - mean
            var = jnp.mean(cen * cen, axis=-1, keepdims=True)
            z = cen * lax.rsqrt(var + 1e-5)
            abuf[r_dst, :] = (z * norms[0:1, :] + norms[1:2, :]).astype(BF16)
            m_all[r_dst, :] = (z * norms[2:3, :] + norms[3:4, :]).astype(BF16)

        for c in small:
            c.wait()

        def own_step(i, carry):
            norm_rows(x_own, pl.ds(pl.multiple_of(i * LR, LR), LR), rows(t, i * LR, LR))
            return carry

        lax.fori_loop(0, TB // LR, own_step, 0)
        from_partner.wait_recv()

        def blk_step(i, carry):
            r = rows(partner, i * LR, LR)
            norm_rows(abuf, r, r)
            return carry

        lax.fori_loop(0, TB // LR, blk_step, 0)

        def norm_piece(blk, i):
            r = rows(blk, i * PROWS, PROWS)
            norm_rows(abuf, r, r)

        def qkv_half(p, r0):
            r = pl.ds(r0, HALF)
            qkv[p, r, :] = jnp.dot(abuf[r, :], ring[p], preferred_element_type=F32).astype(BF16)

        def qkv_last(r0):
            r = pl.ds(r0, HALF)
            p = N_QKV - 1
            n = NB // 2
            qkv[p, r, pl.ds(0, n)] = jnp.dot(abuf[r, :], ring[p, :, pl.ds(0, n)], preferred_element_type=F32).astype(BF16)

        def near_step(p, carry):
            wait_ring(p)

            @pl.when(p == 3)
            def _():
                from_cross[0].wait_recv()
                forward[0].start()

            @pl.when(p == 6)
            def _():
                from_cross[1].wait_recv()
                forward[1].start()
            qkv_half(p, near0)
            return carry

        lax.fori_loop(0, N_QKV - 1, near_step, 0)
        wait_ring(N_QKV - 1, NB // 2)
        qkv_last(near0)

        lane = lax.broadcasted_iota(jnp.int32, (HD, T), 0)
        half = jnp.where(lane < HD // 2, lane, lane - HD // 2).astype(F32)
        inv_freq = jnp.exp(half * (-2.0 / HD) * 9.210340371976184)
        ang = pos_v[...].astype(F32) * inv_freq
        cos_t[...] = jnp.cos(ang).T
        sin_t[...] = jnp.where(lane < HD // 2, -jnp.sin(ang), jnp.sin(ang)).T
        acc[...] = jnp.zeros_like(acc)

        forward[0].wait_send()
        norm_piece(cross, 0)
        from_fwd[0].wait_recv()
        norm_piece(diag, 0)
        for i in range(2, NPIECE):
            from_cross[i].wait_recv()
            forward[i].start()
            forward[i - 1].wait_send()
            norm_piece(cross, i - 1)
            from_fwd[i - 1].wait_recv()
            norm_piece(diag, i - 1)
        forward[NPIECE - 1].wait_send()
        norm_piece(cross, NPIECE - 1)
        from_fwd[NPIECE - 1].wait_recv()
        norm_piece(diag, NPIECE - 1)

        def far_step(i, carry):
            for p in (2 * i, 2 * i + 1):
                qkv_half(p, far0)
            for p in (2 * i, 2 * i + 1):
                issue(p + RING)
            return carry

        lax.fori_loop(0, N_QKV // 2 - 1, far_step, 0)
        qkv_half(N_QKV - 2, far0)
        qkv_last(far0)
        for p in (N_QKV - 2, N_QKV - 1):
            issue(jnp.int32(p + RING))

        def rot(u):
            u = u.astype(F32)
            return (u * cos_t[...] + pltpu.roll(u, HD // 2, 1) * sin_t[...]).astype(BF16)

        def head(h, dot_a, dot_b):
            qp = 2 + h // 2
            qc = pl.multiple_of(lax.rem(h, 2) * 2 * HD, 2 * HD)
            vp = jnp.where(h < 8, h // 4, N_QKV - 1)
            q = rot(qkv[qp, :, pl.ds(qc, HD)])
            k = rot(qkv[qp, :, pl.ds(qc + HD, HD)])
            first = dot_a()
            sc = lax.dot_general(q, k, (((1,), (1,)), ((), ())), preferred_element_type=F32) * (HD ** -0.5)
            second = dot_b()
            mask = lax.broadcasted_iota(jnp.int32, (T, T), 1) <= lax.broadcasted_iota(jnp.int32, (T, T), 0)
            sc = jnp.where(mask, sc, -1e30)
            e = jnp.exp(sc - jnp.max(sc, axis=-1, keepdims=True))
            pr = (e * (1.0 / jnp.sum(e, axis=-1, keepdims=True))).astype(BF16)
            v = qkv[vp, :, pl.ds(pl.multiple_of(lax.rem(h, 4) * HD, HD), HD)]
            ctx[:, cols(h, HD)] = jnp.dot(pr, v, preferred_element_type=F32).astype(BF16)
            return first + second

        def up_step(i, carry):
            h0 = 2 * i
            g0 = h0 + UP0
            ss = [wait_ring(g0), wait_ring(g0 + 1)]

            @pl.when(i >= 1)
            def _():
                issue(g0 - 2 + RING)
                issue(g0 - 1 + RING)

            def part_dot(s, lo):
                r = pl.ds(lo, KC)
                return lambda: jnp.dot(m_all[:, r], ring[s, r, :], preferred_element_type=F32)
            gelu_store(acc[...], jnp.maximum(h0 - 1, 0))
            u0 = head(h0, part_dot(ss[0], 0), part_dot(ss[0], KC))
            gelu_store(u0, h0)
            u1 = head(h0 + 1, part_dot(ss[1], 0), part_dot(ss[1], KC))
            acc[...] = u1
            return carry

        lax.fori_loop(0, N_UP // 2, up_step, 0)
        gelu_store(acc[...], N_UP - 1)

    def back(part):
        def a_copy(j, i):
            blk = partner if i == 0 else diag
            return remote(part.at[j, rows(blk)], ra.at[lax.rem(j, RA), i], a_send.at[j, i], a_recv.at[j, i], partner)

        def b_copy(j):
            return remote(sb.at[lax.rem(j, SB)], rb.at[j], b_send.at[j], b_recv.at[j], cross)

        def do_a(j):
            for i in range(2):
                a_copy(j, i).start()

        def do_b(j):
            for i in range(2):
                a_copy(j, i).wait_recv()
            r = lax.rem(j, RA)

            @pl.when(j >= SB)
            def _():
                b_copy(j - SB).wait_send()
            sb[lax.rem(j, SB)] = (part[j, rows(cross), :] + ra[r, 1]).astype(BF16)
            b_copy(j).start()
            part[j, rows(t), :] = part[j, rows(t), :] + ra[r, 0]

        def out_copy(j):
            return local(x_own.at[:, cols(j)], out_hbm.at[:, cols(j)], out_sem.at[j])

        def do_c(j):
            b_copy(j).wait_recv()
            x_own[:, cols(j)] = (x_own[:, cols(j)].astype(F32) + (part[j, rows(t), :] + rb[j].astype(F32))).astype(BF16)
            out_copy(j).start()

        def out_dot(j, s):
            return part[j] + jnp.dot(abuf[...], ring[s], preferred_element_type=F32)

        def refill(j):
            @pl.when(j + DN0 + RING < N_ITEMS)
            def _():
                issue(j + DN0 + RING)

        for g in (WO0 - 2, WO0 - 1):
            issue(jnp.int32(g + RING))

        def wo_block(q, h, s):
            part[4 * q + h] = jnp.dot(ctx[...], ring[s, pl.ds(h * CTX, CTX), :], preferred_element_type=F32)

        def wo_step(q, carry):
            s = wait_ring(WO0 + q)
            for h in range(4):
                wo_block(q, h, s)
            issue(WO0 + q + RING)
            return carry

        lax.fori_loop(0, N_WO - 1, wo_step, 0)
        s = (DN0 - 1) % RING
        local(wup_hbm.at[pl.ds(0, 2 * CTX), pl.ds(0, NB)], ring.at[s, pl.ds(0, 2 * CTX), :], ring_sem.at[s]).wait()
        for h in range(2):
            wo_block(N_WO - 1, h, s)
        issue(jnp.int32(DN0 - 1 + RING))

        def dn_step(j, carry):
            s = wait_ring(j + DN0)

            @pl.when(j >= 1)
            def _():
                do_a(j - 1)
                refill(j - 1)

            @pl.when(j >= 2)
            def _():
                do_b(j - 2)

            @pl.when(j >= 4)
            def _():
                do_c(j - 4)
            part[j] = out_dot(j, s)
            return carry

        lax.fori_loop(0, N_DN, dn_step, 0)
        do_a(N_DN - 1)
        do_b(N_DN - 2)
        do_c(N_DN - 4)
        do_b(N_DN - 1)
        for j in range(N_DN - 3, N_DN):
            do_c(j)

        for j in range(N_DN - SB, N_DN):
            b_copy(j).wait_send()

        def drain(j, carry):
            for i in range(2):
                a_copy(j, i).wait_send()
            out_copy(j).wait()
            return carry

        lax.fori_loop(0, N_DN, drain, 0)

    pl.run_scoped(front, pltpu.VMEM((T, D), BF16), pltpu.VMEM((N_QKV, T, NB), BF16),
                  pltpu.VMEM((T, HD), F32), pltpu.VMEM((T, HD), F32), pltpu.VMEM((T, NB), F32))
    for c in to_cross + [to_partner]:
        c.wait_send()
    pl.run_scoped(back, pltpu.VMEM((N_DN, T, NB), F32))


def solution(mesh):
    def local_layer(hidden_blk, attn_gain, attn_bias, mlp_gain, mlp_bias, w_qkv, w_out, w_up, w_down, positions):
        args = (hidden_blk.reshape(TB, D), attn_gain.reshape(1, D), attn_bias.reshape(1, D), mlp_gain.reshape(1, D),
                mlp_bias.reshape(1, D), jnp.transpose(w_qkv, (1, 0, 2)), w_out, w_up, w_down, positions.reshape(1, T))
        dma = pltpu.SemaphoreType.DMA
        out = pl.pallas_call(
            body,
            out_shape=jax.ShapeDtypeStruct((TB, D), BF16),
            in_specs=[pl.BlockSpec(memory_space=pl.ANY)] * 10,
            out_specs=pl.BlockSpec(memory_space=pl.ANY),
            scratch_shapes=[
                pltpu.VMEM((TB, D), BF16),
                pltpu.VMEM((T, D), BF16),
                pltpu.VMEM((T, CTX), BF16),
                pltpu.VMEM((4, D), F32),
                pltpu.VMEM((1, T), jnp.int32),
                pltpu.VMEM((RING, D, NB), BF16),
                pltpu.VMEM((RA, 2, TB, NB), F32),
                pltpu.VMEM((SB, TB, NB), BF16),
                pltpu.VMEM((N_DN, TB, NB), BF16),
                dma((RING,)), dma((6,)), dma((1,)), dma((1,)), dma((NPIECE,)), dma((NPIECE,)),
                dma((NPIECE,)), dma((NPIECE,)), dma((N_DN, 2)), dma((N_DN, 2)), dma((N_DN,)), dma((N_DN,)), dma((N_DN,)),
            ],
            compiler_params=pltpu.CompilerParams(collective_id=0, has_side_effects=True, vmem_limit_bytes=67043328),
            cost_estimate=pl.CostEstimate(flops=40_300_000_000, bytes_accessed=158_000_000, transcendentals=2_000_000),
            name="layer",
        )(*args)
        return out.reshape(1, TB, D)

    return jax.shard_map(local_layer, mesh=mesh,
                         in_specs=(P('dp', 'tp', None), P(), P(), P(), P(), P(None, 'tp', None), P('tp', None), P(None, 'tp'), P('tp', None), P()),
                         out_specs=P('dp', 'tp', None), check_vma=False)
```

```python
import jax
import jax.numpy as jnp
from jax import lax
from jax.experimental import pallas as pl
from jax.experimental.pallas import tpu as pltpu
from jax.sharding import PartitionSpec as P

MESH = pl.DeviceIdType.MESH
F32 = jnp.float32
BF16 = jnp.bfloat16

D = 5120
T = 256
TB = 64
HD = 128
G = 10
FF = 5120
NB = 512
CTX = G * HD
RING = 9
SB = 4
N_QKV = 8
N_UP = FF // NB
N_DN = D // NB
UP0 = N_QKV
WO0 = UP0 + N_UP
N_WO = 3
DN0 = WO0 + N_WO
N_ITEMS = DN0 + N_DN
NPIECE = 4
PROWS = TB // NPIECE
HALF = 2 * TB
RA = 5
KC = 2560


def body(x_hbm, ga_hbm, ba_hbm, gm_hbm, bm_hbm, wqkv_hbm, wo_hbm, wup_hbm, wdn_hbm, pos_hbm,
         out_hbm,
         x_own, abuf, ctx, norms, pos_v,
         ring, ra, sb, rb,
         ring_sem, misc_sem, x_send, x_recv, c_send, c_recv, f_send, f_recv,
         a_send, a_recv, b_send, b_recv, out_sem):
    t = lax.axis_index("tp")
    partner = t + 1 - 2 * lax.rem(t, 2)
    cross = lax.rem(t + 2, 4)
    diag = lax.rem(partner + 2, 4)
    near0 = pl.multiple_of((t // 2) * HALF, HALF)
    far0 = pl.multiple_of((1 - t // 2) * HALF, HALF)

    def local(src, dst, sem):
        return pltpu.make_async_copy(src, dst, sem)

    def remote(src, dst, ssem, rsem, dev):
        return pltpu.make_async_remote_copy(src_ref=src, dst_ref=dst, send_sem=ssem, recv_sem=rsem,
                                            device_id={"tp": dev}, device_id_type=MESH)

    def rows(blk, start=0, n=TB):
        return pl.ds(pl.multiple_of(blk * TB + start, 16), n)

    def cols(i, n=NB):
        return pl.ds(pl.multiple_of(i * n, n), n)

    def issue_qkv(p):
        if p in (0, 1, 7):
            j = {0: 0, 1: 1, 7: 2}[p]
            for h in range(4 if j < 2 else 2):
                local(wqkv_hbm.at[4 * j + h, :, pl.ds(2 * HD, HD)], ring.at[p, :, pl.ds(h * HD, HD)], ring_sem.at[p]).start()
        else:
            for h in range(2):
                local(wqkv_hbm.at[2 * (p - 2) + h, :, pl.ds(0, 2 * HD)], ring.at[p, :, pl.ds(h * 2 * HD, 2 * HD)], ring_sem.at[p]).start()

    def issue(g):
        s = lax.rem(g, RING)

        @pl.when(g < WO0)
        def _():
            local(wup_hbm.at[:, cols(g - UP0)], ring.at[s], ring_sem.at[s]).start()

        for q in range(N_WO):
            @pl.when(g == WO0 + q)
            def _(q=q):
                for h in range(4 if q < 2 else 2):
                    local(wo_hbm.at[:, pl.ds((4 * q + h) * NB, NB)], ring.at[(WO0 + q) % RING, pl.ds(h * CTX, CTX), :],
                          ring_sem.at[(WO0 + q) % RING]).start()

        @pl.when(jnp.logical_and(g >= DN0, g < N_ITEMS))
        def _():
            local(wdn_hbm.at[:, cols(g - DN0)], ring.at[s], ring_sem.at[s]).start()

    def wait_ring(g, n=NB):
        s = lax.rem(g, RING)
        local(wup_hbm.at[:, pl.ds(0, n)], ring.at[s, :, pl.ds(0, n)], ring_sem.at[s]).wait()
        return s

    xc = local(x_hbm, x_own, misc_sem.at[0])
    xc.start()
    small = [local(h, norms.at[pl.ds(i, 1), :], misc_sem.at[1 + i]) for i, h in enumerate((ga_hbm, ba_hbm, gm_hbm, bm_hbm))]
    small.append(local(pos_hbm, pos_v, misc_sem.at[5]))
    for c in small:
        c.start()
    barrier = pltpu.get_barrier_semaphore()
    for dev in (partner, cross):
        pl.semaphore_signal(barrier, inc=1, device_id={"tp": dev}, device_id_type=MESH)
    for p in range(N_QKV):
        issue_qkv(p)
    issue(jnp.int32(UP0))
    xc.wait()
    pl.semaphore_wait(barrier, 2)

    to_cross = [remote(x_own.at[pl.ds(i * PROWS, PROWS)], abuf.at[rows(t, i * PROWS, PROWS)], c_send.at[i], c_recv.at[i], cross) for i in range(NPIECE)]
    for c in to_cross:
        c.start()
    to_partner = remote(x_own, abuf.at[rows(t)], x_send.at[0], x_recv.at[0], partner)
    to_partner.start()

    def cross_rows(i):
        return abuf.at[rows(cross, i * PROWS, PROWS)]

    def diag_rows(i):
        return abuf.at[rows(diag, i * PROWS, PROWS)]

    from_cross = [remote(cross_rows(i), cross_rows(i), c_send.at[i], c_recv.at[i], cross) for i in range(NPIECE)]
    from_partner = remote(abuf.at[rows(partner)], abuf.at[rows(partner)], x_send.at[0], x_recv.at[0], partner)
    forward = [remote(cross_rows(i), cross_rows(i), f_send.at[i], f_recv.at[i], partner) for i in range(NPIECE)]
    from_fwd = [remote(diag_rows(i), diag_rows(i), f_send.at[i], f_recv.at[i], partner) for i in range(NPIECE)]

    def gelu_store(u, j):
        abuf[:, cols(j)] = (0.5 * u * (1.0 + lax.erf(u * 0.7071067811865476))).astype(BF16)

    def front(m_all, qkv, cos_t, sin_t, acc):
        LR = 16

        def norm_rows(src, r_src, r_dst):
            xr = src[r_src, :].astype(F32)
            mean = jnp.mean(xr, axis=-1, keepdims=True)
            cen = xr - mean
            var = jnp.mean(cen * cen, axis=-1, keepdims=True)
            z = cen * lax.rsqrt(var + 1e-5)
            abuf[r_dst, :] = (z * norms[0:1, :] + norms[1:2, :]).astype(BF16)
            m_all[r_dst, :] = (z * norms[2:3, :] + norms[3:4, :]).astype(BF16)

        for c in small:
            c.wait()

        def own_step(i, carry):
            norm_rows(x_own, pl.ds(pl.multiple_of(i * LR, LR), LR), rows(t, i * LR, LR))
            return carry

        lax.fori_loop(0, TB // LR, own_step, 0)
        from_partner.wait_recv()

        def blk_step(i, carry):
            r = rows(partner, i * LR, LR)
            norm_rows(abuf, r, r)
            return carry

        lax.fori_loop(0, TB // LR, blk_step, 0)

        def norm_piece(blk, i):
            r = rows(blk, i * PROWS, PROWS)
            norm_rows(abuf, r, r)

        def qkv_half(p, r0):
            r = pl.ds(r0, HALF)
            qkv[p, r, :] = jnp.dot(abuf[r, :], ring[p], preferred_element_type=F32).astype(BF16)

        def qkv_last(r0):
            r = pl.ds(r0, HALF)
            p = N_QKV - 1
            n = NB // 2
            qkv[p, r, pl.ds(0, n)] = jnp.dot(abuf[r, :], ring[p, :, pl.ds(0, n)], preferred_element_type=F32).astype(BF16)

        def near_step(p, carry):
            wait_ring(p)

            @pl.when(p == 3)
            def _():
                from_cross[0].wait_recv()
                forward[0].start()

            @pl.when(p == 6)
            def _():
                from_cross[1].wait_recv()
                forward[1].start()
            qkv_half(p, near0)
            return carry

        lax.fori_loop(0, N_QKV - 1, near_step, 0)
        wait_ring(N_QKV - 1, NB // 2)
        qkv_last(near0)

        lane = lax.broadcasted_iota(jnp.int32, (HD, T), 0)
        half = jnp.where(lane < HD // 2, lane, lane - HD // 2).astype(F32)
        inv_freq = jnp.exp(half * (-2.0 / HD) * 9.210340371976184)
        ang = pos_v[...].astype(F32) * inv_freq
        cos_t[...] = jnp.cos(ang).T
        sin_t[...] = jnp.where(lane < HD // 2, -jnp.sin(ang), jnp.sin(ang)).T
        acc[...] = jnp.zeros_like(acc)

        forward[0].wait_send()
        norm_piece(cross, 0)
        from_fwd[0].wait_recv()
        norm_piece(diag, 0)
        for i in range(2, NPIECE):
            from_cross[i].wait_recv()
            forward[i].start()
            forward[i - 1].wait_send()
            norm_piece(cross, i - 1)
            from_fwd[i - 1].wait_recv()
            norm_piece(diag, i - 1)
        forward[NPIECE - 1].wait_send()
        norm_piece(cross, NPIECE - 1)
        from_fwd[NPIECE - 1].wait_recv()
        norm_piece(diag, NPIECE - 1)

        def far_step(i, carry):
            for p in (2 * i, 2 * i + 1):
                qkv_half(p, far0)
            for p in (2 * i, 2 * i + 1):
                issue(p + RING)
            return carry

        lax.fori_loop(0, N_QKV // 2 - 1, far_step, 0)
        qkv_half(N_QKV - 2, far0)
        qkv_last(far0)
        for p in (N_QKV - 2, N_QKV - 1):
            issue(jnp.int32(p + RING))

        def rot(u):
            u = u.astype(F32)
            return (u * cos_t[...] + pltpu.roll(u, HD // 2, 1) * sin_t[...]).astype(BF16)

        def head(h, dot_a, dot_b):
            qp = 2 + h // 2
            qc = pl.multiple_of(lax.rem(h, 2) * 2 * HD, 2 * HD)
            vp = jnp.where(h < 8, h // 4, N_QKV - 1)
            q = rot(qkv[qp, :, pl.ds(qc, HD)])
            k = rot(qkv[qp, :, pl.ds(qc + HD, HD)])
            first = dot_a()
            sc = lax.dot_general(q, k, (((1,), (1,)), ((), ())), preferred_element_type=F32) * (HD ** -0.5)
            second = dot_b()
            mask = lax.broadcasted_iota(jnp.int32, (T, T), 1) <= lax.broadcasted_iota(jnp.int32, (T, T), 0)
            sc = jnp.where(mask, sc, -1e30)
            e = jnp.exp(sc - jnp.max(sc, axis=-1, keepdims=True))
            pr = (e * (1.0 / jnp.sum(e, axis=-1, keepdims=True))).astype(BF16)
            v = qkv[vp, :, pl.ds(pl.multiple_of(lax.rem(h, 4) * HD, HD), HD)]
            ctx[:, cols(h, HD)] = jnp.dot(pr, v, preferred_element_type=F32).astype(BF16)
            return first + second

        def up_step(i, carry):
            h0 = 2 * i
            g0 = h0 + UP0
            ss = [wait_ring(g0), wait_ring(g0 + 1)]

            @pl.when(i >= 1)
            def _():
                issue(g0 - 2 + RING)
                issue(g0 - 1 + RING)

            def part_dot(s, lo):
                r = pl.ds(lo, KC)
                return lambda: jnp.dot(m_all[:, r], ring[s, r, :], preferred_element_type=F32)
            gelu_store(acc[...], jnp.maximum(h0 - 1, 0))
            u0 = head(h0, part_dot(ss[0], 0), part_dot(ss[0], KC))
            gelu_store(u0, h0)
            u1 = head(h0 + 1, part_dot(ss[1], 0), part_dot(ss[1], KC))
            acc[...] = u1
            return carry

        lax.fori_loop(0, N_UP // 2, up_step, 0)
        gelu_store(acc[...], N_UP - 1)

    def back(part):
        def a_copy(j, i):
            blk = partner if i == 0 else diag
            return remote(part.at[j, rows(blk)], ra.at[lax.rem(j, RA), i], a_send.at[j, i], a_recv.at[j, i], partner)

        def b_copy(j):
            return remote(sb.at[lax.rem(j, SB)], rb.at[j], b_send.at[j], b_recv.at[j], cross)

        def do_a(j):
            for i in range(2):
                a_copy(j, i).start()

        def do_b(j, late=False):
            for i in range(2):
                a_copy(j, i).wait_recv()
            r = lax.rem(j, RA)
            if late:
                b_copy(j - SB).wait_send()
            else:
                @pl.when(j >= SB)
                def _():
                    b_copy(j - SB).wait_send()
            sb[lax.rem(j, SB)] = (part[j, rows(cross), :] + ra[r, 1]).astype(BF16)
            b_copy(j).start()
            part[j, rows(t), :] = part[j, rows(t), :] + ra[r, 0]

        def out_copy(j):
            return local(x_own.at[:, cols(j)], out_hbm.at[:, cols(j)], out_sem.at[j])

        def do_c(j):
            b_copy(j).wait_recv()
            x_own[:, cols(j)] = (x_own[:, cols(j)].astype(F32) + (part[j, rows(t), :] + rb[j].astype(F32))).astype(BF16)
            out_copy(j).start()

        def out_dot(j, s):
            return part[j] + jnp.dot(abuf[...], ring[s], preferred_element_type=F32)

        def refill(j):
            @pl.when(j + DN0 + RING < N_ITEMS)
            def _():
                issue(j + DN0 + RING)

        for g in (WO0 - 2, WO0 - 1):
            issue(jnp.int32(g + RING))

        def wo_block(q, h, s):
            part[4 * q + h] = jnp.dot(ctx[...], ring[s, pl.ds(h * CTX, CTX), :], preferred_element_type=F32)

        def wo_step(q, carry):
            s = wait_ring(WO0 + q)
            for h in range(4):
                wo_block(q, h, s)
            issue(WO0 + q + RING)
            return carry

        lax.fori_loop(0, N_WO - 1, wo_step, 0)
        s = (DN0 - 1) % RING
        local(wup_hbm.at[pl.ds(0, 2 * CTX), pl.ds(0, NB)], ring.at[s, pl.ds(0, 2 * CTX), :], ring_sem.at[s]).wait()
        for h in range(2):
            wo_block(N_WO - 1, h, s)
        issue(jnp.int32(DN0 - 1 + RING))

        def dn_step(j, carry):
            s = wait_ring(j + DN0)

            @pl.when(j >= 1)
            def _():
                do_a(j - 1)
                refill(j - 1)

            @pl.when(j >= 2)
            def _():
                do_b(j - 2)

            @pl.when(j >= 4)
            def _():
                do_c(j - 4)
            part[j] = out_dot(j, s)
            return carry

        def dn_late(j, carry):
            s = wait_ring(j + DN0)
            do_a(j - 1)
            do_b(j - 2, late=True)
            do_c(j - 4)
            part[j] = out_dot(j, s)
            return carry

        lax.fori_loop(0, SB + 2, dn_step, 0)
        lax.fori_loop(SB + 2, N_DN, dn_late, 0)
        do_a(N_DN - 1)
        do_b(N_DN - 2, late=True)
        do_c(N_DN - 4)
        do_c(N_DN - 3)
        do_b(N_DN - 1, late=True)

        def sent(j, carry):
            for i in range(2):
                a_copy(j, i).wait_send()
            return carry

        def stored(j, carry):
            out_copy(j).wait()
            return carry

        lax.fori_loop(0, N_DN, sent, 0)
        lax.fori_loop(0, N_DN - 3, stored, 0)
        do_c(N_DN - 2)
        for j in range(N_DN - SB, N_DN):
            b_copy(j).wait_send()
        do_c(N_DN - 1)
        lax.fori_loop(N_DN - 3, N_DN, stored, 0)

    pl.run_scoped(front, pltpu.VMEM((T, D), BF16), pltpu.VMEM((N_QKV, T, NB), BF16),
                  pltpu.VMEM((T, HD), F32), pltpu.VMEM((T, HD), F32), pltpu.VMEM((T, NB), F32))
    for c in to_cross + [to_partner]:
        c.wait_send()
    pl.run_scoped(back, pltpu.VMEM((N_DN, T, NB), F32))


def solution(mesh):
    def local_layer(hidden_blk, attn_gain, attn_bias, mlp_gain, mlp_bias, w_qkv, w_out, w_up, w_down, positions):
        args = (hidden_blk.reshape(TB, D), attn_gain.reshape(1, D), attn_bias.reshape(1, D), mlp_gain.reshape(1, D),
                mlp_bias.reshape(1, D), jnp.transpose(w_qkv, (1, 0, 2)), w_out, w_up, w_down, positions.reshape(1, T))
        dma = pltpu.SemaphoreType.DMA
        out = pl.pallas_call(
            body,
            out_shape=jax.ShapeDtypeStruct((TB, D), BF16),
            in_specs=[pl.BlockSpec(memory_space=pl.ANY)] * 10,
            out_specs=pl.BlockSpec(memory_space=pl.ANY),
            scratch_shapes=[
                pltpu.VMEM((TB, D), BF16),
                pltpu.VMEM((T, D), BF16),
                pltpu.VMEM((T, CTX), BF16),
                pltpu.VMEM((4, D), F32),
                pltpu.VMEM((1, T), jnp.int32),
                pltpu.VMEM((RING, D, NB), BF16),
                pltpu.VMEM((RA, 2, TB, NB), F32),
                pltpu.VMEM((SB, TB, NB), BF16),
                pltpu.VMEM((N_DN, TB, NB), BF16),
                dma((RING,)), dma((6,)), dma((1,)), dma((1,)), dma((NPIECE,)), dma((NPIECE,)),
                dma((NPIECE,)), dma((NPIECE,)), dma((N_DN, 2)), dma((N_DN, 2)), dma((N_DN,)), dma((N_DN,)), dma((N_DN,)),
            ],
            compiler_params=pltpu.CompilerParams(collective_id=0, has_side_effects=True, vmem_limit_bytes=67043328),
            cost_estimate=pl.CostEstimate(flops=40_300_000_000, bytes_accessed=158_000_000, transcendentals=2_000_000),
            name="layer",
        )(*args)
        return out.reshape(1, TB, D)

    return jax.shard_map(local_layer, mesh=mesh,
                         in_specs=(P('dp', 'tp', None), P(), P(), P(), P(), P(None, 'tp', None), P('tp', None), P(None, 'tp'), P('tp', None), P()),
                         out_specs=P('dp', 'tp', None), check_vma=False)
```

```python
import jax
import jax.numpy as jnp
from jax import lax
from jax.experimental import pallas as pl
from jax.experimental.pallas import tpu as pltpu
from jax.sharding import PartitionSpec as P

MESH = pl.DeviceIdType.MESH
F32 = jnp.float32
BF16 = jnp.bfloat16

D = 5120
T = 256
TB = 64
HD = 128
G = 10
FF = 5120
NB = 512
CTX = G * HD
RING = 9
SB = 4
N_QKV = 8
N_UP = FF // NB
N_DN = D // NB
UP0 = N_QKV
WO0 = UP0 + N_UP
N_WO = 3
DN0 = WO0 + N_WO
N_ITEMS = DN0 + N_DN
NPIECE = 4
PROWS = TB // NPIECE
HALF = 2 * TB
RA = 5
KC = 2560


def body(x_hbm, ga_hbm, ba_hbm, gm_hbm, bm_hbm, wqkv_hbm, wo_hbm, wup_hbm, wdn_hbm, pos_hbm,
         out_hbm,
         x_own, abuf, ctx, norms, pos_v,
         ring, ra, sb, rb,
         ring_sem, misc_sem, x_send, x_recv, c_send, c_recv, f_send, f_recv,
         a_send, a_recv, b_send, b_recv, out_sem):
    t = lax.axis_index("tp")
    partner = t + 1 - 2 * lax.rem(t, 2)
    cross = lax.rem(t + 2, 4)
    diag = lax.rem(partner + 2, 4)
    near0 = pl.multiple_of((t // 2) * HALF, HALF)
    far0 = pl.multiple_of((1 - t // 2) * HALF, HALF)

    def local(src, dst, sem):
        return pltpu.make_async_copy(src, dst, sem)

    def remote(src, dst, ssem, rsem, dev):
        return pltpu.make_async_remote_copy(src_ref=src, dst_ref=dst, send_sem=ssem, recv_sem=rsem,
                                            device_id={"tp": dev}, device_id_type=MESH)

    def rows(blk, start=0, n=TB):
        return pl.ds(pl.multiple_of(blk * TB + start, 16), n)

    def cols(i, n=NB):
        return pl.ds(pl.multiple_of(i * n, n), n)

    def issue_qkv(p):
        if p in (0, 1, 7):
            j = {0: 0, 1: 1, 7: 2}[p]
            for h in range(4 if j < 2 else 2):
                local(wqkv_hbm.at[4 * j + h, :, pl.ds(2 * HD, HD)], ring.at[p, :, pl.ds(h * HD, HD)], ring_sem.at[p]).start()
        else:
            for h in range(2):
                local(wqkv_hbm.at[2 * (p - 2) + h, :, pl.ds(0, 2 * HD)], ring.at[p, :, pl.ds(h * 2 * HD, 2 * HD)], ring_sem.at[p]).start()

    def issue(g):
        s = lax.rem(g, RING)

        @pl.when(g < WO0)
        def _():
            local(wup_hbm.at[:, cols(g - UP0)], ring.at[s], ring_sem.at[s]).start()

        for q in range(N_WO):
            @pl.when(g == WO0 + q)
            def _(q=q):
                for h in range(4 if q < 2 else 2):
                    local(wo_hbm.at[:, pl.ds((4 * q + h) * NB, NB)], ring.at[(WO0 + q) % RING, pl.ds(h * CTX, CTX), :],
                          ring_sem.at[(WO0 + q) % RING]).start()

        @pl.when(jnp.logical_and(g >= DN0, g < N_ITEMS))
        def _():
            local(wdn_hbm.at[:, cols(g - DN0)], ring.at[s], ring_sem.at[s]).start()

    def wait_ring(g, n=NB):
        s = lax.rem(g, RING)
        local(wup_hbm.at[:, pl.ds(0, n)], ring.at[s, :, pl.ds(0, n)], ring_sem.at[s]).wait()
        return s

    xc = local(x_hbm, x_own, misc_sem.at[0])
    xc.start()
    small = [local(h, norms.at[pl.ds(i, 1), :], misc_sem.at[1 + i]) for i, h in enumerate((ga_hbm, ba_hbm, gm_hbm, bm_hbm))]
    small.append(local(pos_hbm, pos_v, misc_sem.at[5]))
    for c in small:
        c.start()
    barrier = pltpu.get_barrier_semaphore()
    for dev in (partner, cross):
        pl.semaphore_signal(barrier, inc=1, device_id={"tp": dev}, device_id_type=MESH)
    for p in range(N_QKV):
        issue_qkv(p)
    issue(jnp.int32(UP0))
    xc.wait()
    pl.semaphore_wait(barrier, 2)

    to_cross = [remote(x_own.at[pl.ds(i * PROWS, PROWS)], abuf.at[rows(t, i * PROWS, PROWS)], c_send.at[i], c_recv.at[i], cross) for i in range(NPIECE)]
    for c in to_cross:
        c.start()
    to_partner = remote(x_own, abuf.at[rows(t)], x_send.at[0], x_recv.at[0], partner)
    to_partner.start()

    def cross_rows(i):
        return abuf.at[rows(cross, i * PROWS, PROWS)]

    def diag_rows(i):
        return abuf.at[rows(diag, i * PROWS, PROWS)]

    from_cross = [remote(cross_rows(i), cross_rows(i), c_send.at[i], c_recv.at[i], cross) for i in range(NPIECE)]
    from_partner = remote(abuf.at[rows(partner)], abuf.at[rows(partner)], x_send.at[0], x_recv.at[0], partner)
    forward = [remote(cross_rows(i), cross_rows(i), f_send.at[i], f_recv.at[i], partner) for i in range(NPIECE)]
    from_fwd = [remote(diag_rows(i), diag_rows(i), f_send.at[i], f_recv.at[i], partner) for i in range(NPIECE)]

    def gelu_store(u, j):
        abuf[:, cols(j)] = (0.5 * u * (1.0 + lax.erf(u * 0.7071067811865476))).astype(BF16)

    def front(m_all, qkv, cos_t, sin_t, acc):
        LR = 16

        def norm_rows(src, r_src, r_dst):
            xr = src[r_src, :].astype(F32)
            mean = jnp.mean(xr, axis=-1, keepdims=True)
            cen = xr - mean
            var = jnp.mean(cen * cen, axis=-1, keepdims=True)
            z = cen * lax.rsqrt(var + 1e-5)
            abuf[r_dst, :] = (z * norms[0:1, :] + norms[1:2, :]).astype(BF16)
            m_all[r_dst, :] = (z * norms[2:3, :] + norms[3:4, :]).astype(BF16)

        for c in small:
            c.wait()

        def own_step(i, carry):
            norm_rows(x_own, pl.ds(pl.multiple_of(i * LR, LR), LR), rows(t, i * LR, LR))
            return carry

        lax.fori_loop(0, TB // LR, own_step, 0)
        from_partner.wait_recv()

        def blk_step(i, carry):
            r = rows(partner, i * LR, LR)
            norm_rows(abuf, r, r)
            return carry

        lax.fori_loop(0, TB // LR, blk_step, 0)

        def norm_piece(blk, i):
            r = rows(blk, i * PROWS, PROWS)
            norm_rows(abuf, r, r)

        def qkv_half(p, r0):
            r = pl.ds(r0, HALF)
            qkv[p, r, :] = jnp.dot(abuf[r, :], ring[p], preferred_element_type=F32).astype(BF16)

        def qkv_last(r0):
            r = pl.ds(r0, HALF)
            p = N_QKV - 1
            n = NB // 2
            qkv[p, r, pl.ds(0, n)] = jnp.dot(abuf[r, :], ring[p, :, pl.ds(0, n)], preferred_element_type=F32).astype(BF16)

        def near_step(p, carry):
            wait_ring(p)

            @pl.when(p == 3)
            def _():
                from_cross[0].wait_recv()
                forward[0].start()

            @pl.when(p == 6)
            def _():
                from_cross[1].wait_recv()
                forward[1].start()
            qkv_half(p, near0)
            return carry

        lax.fori_loop(0, N_QKV - 1, near_step, 0)
        wait_ring(N_QKV - 1, NB // 2)
        qkv_last(near0)

        lane = lax.broadcasted_iota(jnp.int32, (HD, T), 0)
        half = jnp.where(lane < HD // 2, lane, lane - HD // 2).astype(F32)
        inv_freq = jnp.exp(half * (-2.0 / HD) * 9.210340371976184)
        ang = pos_v[...].astype(F32) * inv_freq
        cos_t[...] = jnp.cos(ang).T
        sin_t[...] = jnp.where(lane < HD // 2, -jnp.sin(ang), jnp.sin(ang)).T
        acc[...] = jnp.zeros_like(acc)

        forward[0].wait_send()
        norm_piece(cross, 0)
        from_fwd[0].wait_recv()
        norm_piece(diag, 0)
        for i in range(2, NPIECE):
            from_cross[i].wait_recv()
            forward[i].start()
            forward[i - 1].wait_send()
            norm_piece(cross, i - 1)
            from_fwd[i - 1].wait_recv()
            norm_piece(diag, i - 1)
        forward[NPIECE - 1].wait_send()
        norm_piece(cross, NPIECE - 1)
        from_fwd[NPIECE - 1].wait_recv()
        norm_piece(diag, NPIECE - 1)

        def far_step(i, carry):
            for p in (2 * i, 2 * i + 1):
                qkv_half(p, far0)
            for p in (2 * i, 2 * i + 1):
                issue(p + RING)
            return carry

        lax.fori_loop(0, N_QKV // 2 - 1, far_step, 0)
        qkv_half(N_QKV - 2, far0)
        qkv_last(far0)
        for p in (N_QKV - 2, N_QKV - 1):
            issue(jnp.int32(p + RING))

        def rot(u):
            u = u.astype(F32)
            return (u * cos_t[...] + pltpu.roll(u, HD // 2, 1) * sin_t[...]).astype(BF16)

        def head(h, dot_a, dot_b):
            qp = 2 + h // 2
            qc = pl.multiple_of(lax.rem(h, 2) * 2 * HD, 2 * HD)
            vp = jnp.where(h < 8, h // 4, N_QKV - 1)
            q = rot(qkv[qp, :, pl.ds(qc, HD)])
            k = rot(qkv[qp, :, pl.ds(qc + HD, HD)])
            first = dot_a()
            sc = lax.dot_general(q, k, (((1,), (1,)), ((), ())), preferred_element_type=F32) * (HD ** -0.5)
            second = dot_b()
            mask = lax.broadcasted_iota(jnp.int32, (T, T), 1) <= lax.broadcasted_iota(jnp.int32, (T, T), 0)
            sc = jnp.where(mask, sc, -1e30)
            e = jnp.exp(sc - jnp.max(sc, axis=-1, keepdims=True))
            pr = (e * (1.0 / jnp.sum(e, axis=-1, keepdims=True))).astype(BF16)
            v = qkv[vp, :, pl.ds(pl.multiple_of(lax.rem(h, 4) * HD, HD), HD)]
            ctx[:, cols(h, HD)] = jnp.dot(pr, v, preferred_element_type=F32).astype(BF16)
            return first + second

        def up_step(i, carry):
            h0 = 2 * i
            g0 = h0 + UP0
            ss = [wait_ring(g0), wait_ring(g0 + 1)]

            @pl.when(i >= 1)
            def _():
                issue(g0 - 2 + RING)
                issue(g0 - 1 + RING)

            def part_dot(s, lo):
                r = pl.ds(lo, KC)
                return lambda: jnp.dot(m_all[:, r], ring[s, r, :], preferred_element_type=F32)
            gelu_store(acc[...], jnp.maximum(h0 - 1, 0))
            u0 = head(h0, part_dot(ss[0], 0), part_dot(ss[0], KC))
            gelu_store(u0, h0)
            u1 = head(h0 + 1, part_dot(ss[1], 0), part_dot(ss[1], KC))
            acc[...] = u1
            return carry

        lax.fori_loop(0, N_UP // 2, up_step, 0)
        gelu_store(acc[...], N_UP - 1)

    def back(part):
        chip, core = t // 2, lax.rem(t, 2)

        def a_copy(j):
            return remote(part.at[j, :, 1 - core], ra.at[lax.rem(j, RA)], a_send.at[j], a_recv.at[j], partner)

        def b_copy(j):
            return remote(sb.at[lax.rem(j, SB)], rb.at[j], b_send.at[lax.rem(j, SB)], b_recv.at[j], cross)

        def do_a(j):
            a_copy(j).start()

        def do_b(j, late=False):
            a_copy(j).wait_recv()
            r = lax.rem(j, RA)
            if late:
                b_copy(j - SB).wait_send()
            else:
                @pl.when(j >= SB)
                def _():
                    b_copy(j - SB).wait_send()
            sb[lax.rem(j, SB)] = (part[j, 1 - chip, core] + ra[r, 1 - chip]).astype(BF16)
            b_copy(j).start()
            part[j, chip, core] = part[j, chip, core] + ra[r, chip]

        def out_copy(j):
            return local(x_own.at[:, cols(j)], out_hbm.at[:, cols(j)], out_sem.at[j])

        def do_c(j):
            b_copy(j).wait_recv()
            x_own[:, cols(j)] = (x_own[:, cols(j)].astype(F32) + (part[j, chip, core] + rb[j].astype(F32))).astype(BF16)
            out_copy(j).start()

        def out_dot(j, s):
            return part[j] + jnp.dot(abuf[...], ring[s], preferred_element_type=F32).reshape(2, 2, TB, NB)

        def refill(j):
            @pl.when(j + DN0 + RING < N_ITEMS)
            def _():
                issue(j + DN0 + RING)

        for g in (WO0 - 2, WO0 - 1):
            issue(jnp.int32(g + RING))

        def wo_block(q, h, s):
            part[4 * q + h] = jnp.dot(ctx[...], ring[s, pl.ds(h * CTX, CTX), :], preferred_element_type=F32).reshape(2, 2, TB, NB)

        def wo_step(q, carry):
            s = wait_ring(WO0 + q)
            for h in range(4):
                wo_block(q, h, s)
            issue(WO0 + q + RING)
            return carry

        lax.fori_loop(0, N_WO - 1, wo_step, 0)
        s = (DN0 - 1) % RING
        local(wup_hbm.at[pl.ds(0, 2 * CTX), pl.ds(0, NB)], ring.at[s, pl.ds(0, 2 * CTX), :], ring_sem.at[s]).wait()
        for h in range(2):
            wo_block(N_WO - 1, h, s)
        issue(jnp.int32(DN0 - 1 + RING))

        def dn_step(j, carry):
            s = wait_ring(j + DN0)

            @pl.when(j >= 1)
            def _():
                do_a(j - 1)
                refill(j - 1)

            @pl.when(j >= 2)
            def _():
                do_b(j - 2)

            @pl.when(j >= 4)
            def _():
                do_c(j - 4)
            part[j] = out_dot(j, s)
            return carry

        def dn_late(j, carry):
            s = wait_ring(j + DN0)
            do_a(j - 1)
            do_b(j - 2, late=True)
            do_c(j - 4)
            part[j] = out_dot(j, s)
            return carry

        lax.fori_loop(0, SB + 2, dn_step, 0)
        lax.fori_loop(SB + 2, N_DN, dn_late, 0)
        do_a(N_DN - 1)
        do_b(N_DN - 2, late=True)
        do_c(N_DN - 4)
        do_c(N_DN - 3)
        do_b(N_DN - 1, late=True)

        def sent(j, carry):
            a_copy(j).wait_send()
            return carry

        def stored(j, carry):
            out_copy(j).wait()
            return carry

        lax.fori_loop(0, N_DN, sent, 0)
        lax.fori_loop(0, N_DN - 3, stored, 0)
        do_c(N_DN - 2)
        for j in range(N_DN - SB, N_DN):
            b_copy(j).wait_send()
        do_c(N_DN - 1)
        lax.fori_loop(N_DN - 3, N_DN, stored, 0)

    pl.run_scoped(front, pltpu.VMEM((T, D), BF16), pltpu.VMEM((N_QKV, T, NB), BF16),
                  pltpu.VMEM((T, HD), F32), pltpu.VMEM((T, HD), F32), pltpu.VMEM((T, NB), F32))
    for c in to_cross + [to_partner]:
        c.wait_send()
    pl.run_scoped(back, pltpu.VMEM((N_DN, 2, 2, TB, NB), F32))


def solution(mesh):
    def local_layer(hidden_blk, attn_gain, attn_bias, mlp_gain, mlp_bias, w_qkv, w_out, w_up, w_down, positions):
        args = (hidden_blk.reshape(TB, D), attn_gain.reshape(1, D), attn_bias.reshape(1, D), mlp_gain.reshape(1, D),
                mlp_bias.reshape(1, D), jnp.transpose(w_qkv, (1, 0, 2)), w_out, w_up, w_down, positions.reshape(1, T))
        dma = pltpu.SemaphoreType.DMA
        out = pl.pallas_call(
            body,
            out_shape=jax.ShapeDtypeStruct((TB, D), BF16),
            in_specs=[pl.BlockSpec(memory_space=pl.ANY)] * 10,
            out_specs=pl.BlockSpec(memory_space=pl.ANY),
            scratch_shapes=[
                pltpu.VMEM((TB, D), BF16),
                pltpu.VMEM((T, D), BF16),
                pltpu.VMEM((T, CTX), BF16),
                pltpu.VMEM((4, D), F32),
                pltpu.VMEM((1, T), jnp.int32),
                pltpu.VMEM((RING, D, NB), BF16),
                pltpu.VMEM((RA, 2, TB, NB), F32),
                pltpu.VMEM((SB, TB, NB), BF16),
                pltpu.VMEM((N_DN, TB, NB), BF16),
                dma((RING,)), dma((6,)), dma((1,)), dma((1,)), dma((NPIECE,)), dma((NPIECE,)),
                dma((NPIECE,)), dma((NPIECE,)), dma((N_DN,)), dma((N_DN,)), dma((SB,)), dma((N_DN,)), dma((N_DN,)),
            ],
            compiler_params=pltpu.CompilerParams(collective_id=0, has_side_effects=True, vmem_limit_bytes=67043328),
            cost_estimate=pl.CostEstimate(flops=40_300_000_000, bytes_accessed=158_000_000, transcendentals=2_000_000),
            name="layer",
        )(*args)
        return out.reshape(1, TB, D)

    return jax.shard_map(local_layer, mesh=mesh,
                         in_specs=(P('dp', 'tp', None), P(), P(), P(), P(), P(None, 'tp', None), P('tp', None), P(None, 'tp'), P('tp', None), P()),
                         out_specs=P('dp', 'tp', None), check_vma=False)
```
